512 devices in a mesh: seq: 128 (over z, x_hi, y), head: 4 (over x_lo, core).
Axes of the slice: x: 4 (x_hi: 2, x_lo: 2; x = x_hi * 2 + x_lo), y: 4, z: 16, core: 2. Of those that a mesh axis runs over, the one named last changes fastest.
Arguments:
- q_old: bfloat16 [28672, 2048], P(('seq', 'head')), may hold values from -6 to 6
- k_old: bfloat16 [28672, 1024], P(('seq', 'head')), may hold values from -6 to 6
- value_old_layout: bfloat16 [28672, 1024], P(('seq', 'head')), may hold values from -6 to 6
- dout_old: bfloat16 [28672, 2048], P(('seq', 'head')), may hold values from -6 to 6
- old_offsets: int32 [129], replicated, may hold values from 0 to 16384, as said below
- new_offsets: int32 [129], replicated, may hold values from 0 to 16384, as said below
Outputs:
- attn_out: bfloat16 [28672, 2048], P('seq', 'head')
- grad_query_out: bfloat16 [28672, 2048], P('seq', 'head')
- grad_key_out: bfloat16 [28672, 1024], P('seq', 'head')
- grad_value_out: bfloat16 [28672, 1024], P('seq', 'head')
The draws below stay inside these ranges and needn't reach their ends.
Inputs may be any that keep to these rules, and one draw needn't show every extreme that they name: old_offsets[0] = 0 and old_offsets[128] = 16384; old_offsets[j] lies within 48 of j * 128, at exactly -48 for some j and +48 for some j; some block has exactly 224 positions. new_offsets[0] = 0 and new_offsets[128] = 16384; new_offsets[j] lies within 48 of j * 128, at exactly -48 for some j and +48 for some j; some block has exactly 224 positions; for some j, 96 positions of old block j lie in new block j + 1, and for some j, 96 positions of old block j lie in new block j - 1.
All inputs are finite; a program needn't handle non-finite values.
Results may differ from the reference program's by a relative error of at most 0.02.
Values may be sent and summed in bfloat16 or wider, within the bound.
No kernel may reach another device: no remote copies, remote signals or barrier semaphores. Data moves between devices by JAX's collectives and lax.ppermute only.
A program may use at most 64 MiB of HBM per device.

```python
import jax
import jax.numpy as jnp
from jax import lax

TOK_DEV = 128
ATTEND_WINDOW = 1024
QUERY_HEADS = 16
KEY_VALUE_HEADS = 8
HEAD_SIZE = 128
SLACK = 48
BLOCK_SLOTS = 224
SEQUENCE_TOKENS = 16384
LAYOUT_SLOTS = 28672
N_SEQ = 128


def ownership(key):
    boundary = jnp.arange(N_SEQ + 1, dtype=jnp.int32)
    old_shift = jax.random.randint(jax.random.fold_in(key, 101), (N_SEQ + 1,), -SLACK, SLACK + 1, dtype=jnp.int32)
    new_shift = jax.random.randint(jax.random.fold_in(key, 102), (N_SEQ + 1,), -SLACK, SLACK + 1, dtype=jnp.int32)
    outer_ends = (boundary == 0) | (boundary == N_SEQ)
    old_shift = jnp.where(outer_ends, 0, old_shift)
    new_shift = jnp.where(outer_ends, 0, new_shift)
    wide_block = jax.random.randint(jax.random.fold_in(key, 103), (), 1, N_SEQ // 2 - 1, dtype=jnp.int32)
    late_block = jax.random.randint(jax.random.fold_in(key, 104), (), N_SEQ // 2, N_SEQ, dtype=jnp.int32)
    old_shift = jnp.where(boundary == wide_block, -SLACK, old_shift)
    old_shift = jnp.where(boundary == wide_block + 1, SLACK, old_shift)
    new_shift = jnp.where(boundary == wide_block + 1, -SLACK, new_shift)
    new_shift = jnp.where(boundary == wide_block + 2, SLACK, new_shift)
    old_shift = jnp.where(boundary == late_block, -SLACK, old_shift)
    new_shift = jnp.where(boundary == late_block, SLACK, new_shift)
    return ((boundary * TOK_DEV + old_shift).astype(jnp.int32), (boundary * TOK_DEV + new_shift).astype(jnp.int32))


def draw_old_offsets(key, part):
    return ownership(key)[0]


def draw_new_offsets(key, part):
    return ownership(key)[1]


def draw_q_old(key, part):
    scenery_backdrop = jnp.clip(jax.random.normal(jax.random.fold_in(key, 211), (LAYOUT_SLOTS, QUERY_HEADS * HEAD_SIZE)), -6.0, 6.0)
    return scenery_backdrop.astype(jnp.bfloat16)


def draw_k_old(key, part):
    scenery_backdrop = jnp.clip(jax.random.normal(jax.random.fold_in(key, 212), (LAYOUT_SLOTS, KEY_VALUE_HEADS * HEAD_SIZE)), -6.0, 6.0)
    return scenery_backdrop.astype(jnp.bfloat16)


def level_of(own_key, dims, shards, smallest, high):
    factor_of = 1.0
    for position, parts in shards:
        draws = jax.random.uniform(jax.random.fold_in(jax.random.fold_in(own_key, 6), position), (parts,), jnp.float32, smallest / len(shards), high / len(shards))
        factor_of = factor_of * jnp.repeat(jnp.exp(draws), dims[position] // parts).reshape((-1,) + (1,) * (len(dims) - 1 - position))
    return factor_of


def centred(stream_key, shape, deviation, most, split=(), kind=jnp.bfloat16):
    factor_of = level_of(stream_key, shape, split, -0.22, 0.18) if split else 1.0
    entries = jax.random.normal(stream_key, shape, jnp.float32) * deviation * factor_of
    return jnp.minimum(jnp.maximum(entries, -most), most).astype(kind)


def setup_inputs(seed: int = 0) -> dict:
    key_of = jax.random.split(jax.random.key(seed), 7)
    return {
        "q_old": draw_q_old(jax.random.fold_in(key_of[6], 71), 0),
        "k_old": draw_k_old(jax.random.fold_in(key_of[6], 71), 0),
        "value_old_layout": centred(key_of[2], (LAYOUT_SLOTS, KEY_VALUE_HEADS * HEAD_SIZE), 1.0, 6.0, ((0, 512),)),
        "dout_old": centred(key_of[3], (LAYOUT_SLOTS, QUERY_HEADS * HEAD_SIZE), 1.0, 6.0, ((0, 512),)),
        "old_offsets": draw_old_offsets(jax.random.fold_in(key_of[6], 71), 0),
        "new_offsets": draw_new_offsets(jax.random.fold_in(key_of[6], 71), 0),
    }


query_scale = 168.0 ** -0.5


def gather_rows(slot_data, offsets):
    positions = jnp.arange(SEQUENCE_TOKENS, dtype=jnp.int32)
    owners = jnp.sum((positions[:, None] >= offsets[None, 1:N_SEQ]).astype(jnp.int32), axis=1).astype(jnp.int32)
    picked = (owners * BLOCK_SLOTS + positions - offsets[owners]).astype(jnp.int32)
    return jnp.take(slot_data, picked, axis=0)


def place_rows(full_rows, offsets):
    slot_index = jnp.arange(LAYOUT_SLOTS, dtype=jnp.int32)
    owners = (slot_index // BLOCK_SLOTS).astype(jnp.int32)
    positions = (offsets[owners] + slot_index % BLOCK_SLOTS).astype(jnp.int32)
    is_live = positions < offsets[owners + 1]
    picked = jnp.clip(positions, 0, SEQUENCE_TOKENS - 1).astype(jnp.int32)
    return jnp.where(is_live[:, None], jnp.take(full_rows, picked, axis=0), jnp.zeros((), full_rows.dtype))


def attend_block(queries, grads_out, key_rows, value_rows, allowed):
    heads_per_group = QUERY_HEADS // KEY_VALUE_HEADS
    key_full = jnp.repeat(key_rows.astype(jnp.float32), heads_per_group, axis=1)
    value_full = jnp.repeat(value_rows.astype(jnp.float32), heads_per_group, axis=1)
    query_full = queries.astype(jnp.float32)
    grad_full = grads_out.astype(jnp.float32)
    scores = jnp.einsum("rhd,lhd->hrl", query_full, key_full) * query_scale
    scores = jnp.where(allowed[None], scores, -1e30)
    row_max = jnp.max(scores, axis=2, keepdims=True)
    weights = jnp.where(allowed[None], jnp.exp(scores - row_max), 0.0)
    probabilities = weights / jnp.sum(weights, axis=2, keepdims=True)
    rounded = lax.optimization_barrier(probabilities.astype(jnp.bfloat16)).astype(jnp.float32)
    attn = jnp.einsum("hrl,lhd->rhd", rounded, value_full).astype(jnp.bfloat16)
    attn_full = lax.optimization_barrier(attn).astype(jnp.float32)
    row_delta = jnp.transpose(jnp.sum(grad_full * attn_full, axis=2))[:, :, None]
    grad_prob = jnp.einsum("rhd,lhd->hrl", grad_full, value_full)
    grad_score = (probabilities * (grad_prob - row_delta) * query_scale).astype(jnp.bfloat16)
    score_full = lax.optimization_barrier(grad_score).astype(jnp.float32)
    grad_query = jnp.einsum("hrl,lhd->rhd", score_full, key_full).astype(jnp.bfloat16)
    key_extent = key_rows.shape[0]
    key_gradient = jnp.einsum("hrl,rhd->lhd", score_full, query_full)
    value_gradient = jnp.einsum("hrl,rhd->lhd", rounded, grad_full)
    key_gradient = jnp.sum(key_gradient.reshape(key_extent, KEY_VALUE_HEADS, heads_per_group, HEAD_SIZE), axis=2)
    value_gradient = jnp.sum(value_gradient.reshape(key_extent, KEY_VALUE_HEADS, heads_per_group, HEAD_SIZE), axis=2)
    return attn, grad_query, key_gradient, value_gradient


def reference(q_old, k_old, value_old_layout, dout_old, old_offsets, new_offsets):
    queries = gather_rows(q_old, old_offsets)
    key_rows = gather_rows(k_old, old_offsets)
    value_rows = gather_rows(value_old_layout, old_offsets)
    grads_out = gather_rows(dout_old, old_offsets)
    pad_amount_rows = jnp.zeros((ATTEND_WINDOW, KEY_VALUE_HEADS * HEAD_SIZE), jnp.bfloat16)
    padded_keys = jnp.concatenate([pad_amount_rows, key_rows], axis=0)
    padded_values = jnp.concatenate([pad_amount_rows, value_rows], axis=0)
    key_extent = ATTEND_WINDOW + TOK_DEV

    def block_step(running, block_number):
        key_accumulator, value_accumulator = running
        row_begin = (block_number * TOK_DEV).astype(jnp.int32)
        query_block = lax.dynamic_slice_in_dim(queries, row_begin, TOK_DEV, 0).reshape(TOK_DEV, QUERY_HEADS, HEAD_SIZE)
        grad_block = lax.dynamic_slice_in_dim(grads_out, row_begin, TOK_DEV, 0).reshape(TOK_DEV, QUERY_HEADS, HEAD_SIZE)
        block_of_keys = lax.dynamic_slice_in_dim(padded_keys, row_begin, key_extent, 0).reshape(key_extent, KEY_VALUE_HEADS, HEAD_SIZE)
        block_of_values = lax.dynamic_slice_in_dim(padded_values, row_begin, key_extent, 0).reshape(key_extent, KEY_VALUE_HEADS, HEAD_SIZE)
        query_places = row_begin + jnp.arange(TOK_DEV, dtype=jnp.int32)
        key_places = row_begin - ATTEND_WINDOW + jnp.arange(key_extent, dtype=jnp.int32)
        gap_rows = query_places[:, None] - key_places[None, :]
        allowed = (gap_rows >= 0) & (gap_rows < ATTEND_WINDOW) & (key_places[None, :] >= 0)
        attn, grad_query, key_gradient, value_gradient = attend_block(query_block, grad_block, block_of_keys, block_of_values, allowed)
        key_accumulator = lax.dynamic_update_slice_in_dim(key_accumulator, lax.dynamic_slice_in_dim(key_accumulator, row_begin, key_extent, 0) + key_gradient.reshape(key_extent, KEY_VALUE_HEADS * HEAD_SIZE), row_begin, 0)
        value_accumulator = lax.dynamic_update_slice_in_dim(value_accumulator, lax.dynamic_slice_in_dim(value_accumulator, row_begin, key_extent, 0) + value_gradient.reshape(key_extent, KEY_VALUE_HEADS * HEAD_SIZE), row_begin, 0)
        return (key_accumulator, value_accumulator), (attn.reshape(TOK_DEV, QUERY_HEADS * HEAD_SIZE), grad_query.reshape(TOK_DEV, QUERY_HEADS * HEAD_SIZE))

    start_accumulator = jnp.zeros((SEQUENCE_TOKENS + ATTEND_WINDOW, KEY_VALUE_HEADS * HEAD_SIZE), jnp.float32)
    running, produced = lax.scan(block_step, (start_accumulator, start_accumulator), jnp.arange(SEQUENCE_TOKENS // TOK_DEV, dtype=jnp.int32))
    attn_rows = produced[0].reshape(SEQUENCE_TOKENS, QUERY_HEADS * HEAD_SIZE)
    query_grads = produced[1].reshape(SEQUENCE_TOKENS, QUERY_HEADS * HEAD_SIZE)
    key_grads = running[0][ATTEND_WINDOW:].astype(jnp.bfloat16)
    value_grads = running[1][ATTEND_WINDOW:].astype(jnp.bfloat16)
    return (place_rows(attn_rows, new_offsets), place_rows(query_grads, new_offsets), place_rows(key_grads, new_offsets), place_rows(value_grads, new_offsets))
```

```python
import jax
import jax.numpy as jnp
from jax import lax
from jax.experimental import pallas as pl
from jax.experimental.pallas import tpu as pltpu
from jax.sharding import Mesh, PartitionSpec as P

PAIR = 256
SLOTS = 224
EDGE = 48
HEAD = 128
UNITS = 4
PAIRS = 64
SWAP = PAIR - 80
SCALE = 168.0 ** (-0.5)
LOG2E = 1.4426950408889634
OUTSIDE = -1e30

AXES = ("z", "xh", "yh", "yl", "xl", "c")
PAIR_AXES = ("z", "xh", "yh")
SEQ_AXES = ("z", "xh", "yh", "yl")
GROUP_AXES = ("yl", "xl", "c")
PLANE_AXES = ("xh", "yh")

NT = (((1,), (1,)), ((), ()))
NN = (((1,), (0,)), ((), ()))
TN = (((0,), (0,)), ((), ()))


def dot(a, b, dims):
    return lax.dot_general(a, b, dims, preferred_element_type=jnp.float32)


def pair_index():
    return (lax.axis_index("z") * 2 + lax.axis_index("xh")) * 2 + lax.axis_index("yh")


def vmem():
    return pl.BlockSpec(memory_space=pltpu.VMEM)


def smem():
    return pl.BlockSpec(memory_space=pltpu.SMEM)


def call(kernel, outs, specs, scratch=(), name=None, flops=0):
    many = isinstance(outs, (list, tuple))
    return pl.pallas_call(
        kernel,
        out_shape=outs,
        in_specs=specs,
        out_specs=[vmem() for _ in outs] if many else vmem(),
        scratch_shapes=list(scratch),
        name=name,
        cost_estimate=pl.CostEstimate(flops=flops, bytes_accessed=1 << 20, transcendentals=0),
    )


def shape(*dims, dtype=jnp.bfloat16):
    return jax.ShapeDtypeStruct(dims, dtype)


def picked(rows, source, candidates):
    count = candidates.shape[0]
    columns = lax.broadcasted_iota(jnp.int32, (rows, count), 1)
    chosen = (columns == source).astype(jnp.float32).astype(jnp.bfloat16)
    return dot(chosen, candidates, NN).astype(jnp.bfloat16)


def pack_kernel(first_ref, second_ref, out_ref):
    width = first_ref.shape[1] // 8
    for target in range(8):
        head = (target % 4) * 2 + target // 4
        out_ref[target, :, :width] = first_ref[:, head * width : (head + 1) * width]
        out_ref[target, :, width:] = second_ref[:, head * width : (head + 1) * width]


def pack(first, second, name):
    rows, cols = first.shape
    return call(pack_kernel, shape(8, rows, cols // 4), [vmem(), vmem()], name=name)(first, second)


def edges_kernel(offsets_ref, slots_ref, left_ref, right_ref):
    pair = pair_index()
    first = offsets_ref[2 * pair]
    middle = offsets_ref[2 * pair + 1]
    row = lax.broadcasted_iota(jnp.int32, (2 * EDGE, 1), 0)
    to_left = row + (pair * PAIR - EDGE - first)
    to_right = row + (SLOTS - EDGE + (pair + 1) * PAIR - middle)
    source = jnp.where(row < EDGE, to_left, to_right)
    both = picked(2 * EDGE, source, slots_ref[...])
    left_ref[...] = both[:EDGE]
    right_ref[...] = both[EDGE:]


def even_kernel(offsets_ref, slots_ref, left_ref, right_ref, out_ref):
    pair = pair_index()
    first = offsets_ref[2 * pair]
    middle = offsets_ref[2 * pair + 1]
    last = offsets_ref[2 * pair + 2]
    row = lax.broadcasted_iota(jnp.int32, (PAIR, 1), 0)
    place = row + pair * PAIR
    source = jnp.where(
        place < first,
        2 * SLOTS + row,
        jnp.where(
            place < middle,
            place - first,
            jnp.where(place < last, SLOTS + place - middle, 2 * SLOTS + 2 * EDGE - PAIR + row),
        ),
    )
    width = slots_ref.shape[1]
    candidates = jnp.concatenate(
        [slots_ref[...], left_ref[...], right_ref[...], jnp.zeros((96, width), jnp.bfloat16)], axis=0
    )
    out_ref[...] = picked(PAIR, source, candidates)


def even_rows(slots, offsets, name):
    width = slots.shape[1]
    left, right = call(
        edges_kernel,
        [shape(EDGE, width), shape(EDGE, width)],
        [smem(), vmem()],
        name=name + "_edges",
    )(offsets, slots)
    from_right = lax.ppermute(left, PAIR_AXES, [(i + 1, i) for i in range(PAIRS - 1)])
    from_left = lax.ppermute(right, PAIR_AXES, [(i, i + 1) for i in range(PAIRS - 1)])
    return call(
        even_kernel, shape(PAIR, width), [smem(), vmem(), vmem(), vmem()], name=name + "_even"
    )(offsets, slots, from_left, from_right)


def choose_kernel(own_ref, far_ref, out_ref):
    here = lax.axis_index("xh") * 2 + lax.axis_index("yh")
    for target in range(UNITS):

        @pl.when(here < target)
        def _():
            out_ref[target] = own_ref[...]

        @pl.when(here >= target)
        def _():
            out_ref[target] = far_ref[...]


def attend_kernel(
    rows_ref, own_ref, far_ref, others_ref, out_ref, swap_ref, step_ref, skip_ref,
    given_ref, kept_ref, back_ref, score_ref,
):
    here = lax.axis_index("xh") * 2 + lax.axis_index("yh")
    started = lax.axis_index("z") > 0
    width = 2 * PAIR
    queries = jnp.concatenate([rows_ref[:, :HEAD], rows_ref[:, HEAD : 2 * HEAD]], axis=0)
    grads = jnp.concatenate([rows_ref[:, 2 * HEAD : 3 * HEAD], rows_ref[:, 3 * HEAD :]], axis=0)
    key_row = lax.broadcasted_iota(jnp.int32, (PAIR, width), 0)
    query_row = lax.broadcasted_iota(jnp.int32, (PAIR, width), 1) & (PAIR - 1)
    near = key_row <= query_row
    unit_of = [(here + step) & (UNITS - 1) for step in range(1, UNITS)]
    top = jnp.full((1, width), OUTSIDE, jnp.float32)
    for step, unit in enumerate(unit_of):
        bias = jnp.where((unit < here) | started, 0.0, OUTSIDE)
        score = dot(others_ref[unit, :, :HEAD], queries, NT) * (SCALE * LOG2E) + bias
        score_ref[step * PAIR : (step + 1) * PAIR, :] = score
        top = jnp.maximum(top, jnp.max(score, axis=0, keepdims=True))
    bias = jnp.where(started, 0.0, OUTSIDE)
    score = jnp.where(
        near,
        dot(own_ref[:, :HEAD], queries, NT) * (SCALE * LOG2E),
        dot(far_ref[:, :HEAD], queries, NT) * (SCALE * LOG2E) + bias,
    )
    score_ref[3 * PAIR :, :] = score
    top = jnp.maximum(top, jnp.max(score, axis=0, keepdims=True))
    total = jnp.zeros((1, width), jnp.float32)
    for step in range(UNITS):
        weight = jnp.exp2(score_ref[step * PAIR : (step + 1) * PAIR, :] - top)
        score_ref[step * PAIR : (step + 1) * PAIR, :] = weight
        total = total + jnp.sum(weight, axis=0, keepdims=True)
    share = 1.0 / total
    zero = jnp.zeros((), jnp.bfloat16)
    attn = jnp.zeros((HEAD, width), jnp.float32)
    for step, unit in enumerate(unit_of):
        prob = (score_ref[step * PAIR : (step + 1) * PAIR, :] * share).astype(jnp.bfloat16)
        attn = attn + dot(others_ref[unit, :, HEAD:], prob, TN)
        given_ref[unit, :, HEAD:] = dot(prob, grads, NN).astype(jnp.bfloat16)
    prob = score_ref[3 * PAIR :, :] * share
    prob_own = jnp.where(near, prob, 0.0).astype(jnp.bfloat16)
    prob_far = jnp.where(near, 0.0, prob).astype(jnp.bfloat16)
    attn = attn + dot(own_ref[:, HEAD:], prob_own, TN) + dot(far_ref[:, HEAD:], prob_far, TN)
    kept_ref[:, HEAD:] = dot(prob_own, grads, NN)
    back_ref[:, HEAD:] = dot(prob_far, grads, NN)
    attn = attn.astype(jnp.bfloat16).astype(jnp.float32)
    grads_t = grads.astype(jnp.float32).T
    delta = jnp.sum(attn * grads_t, axis=0, keepdims=True)
    attn_rows = attn.T.astype(jnp.bfloat16)
    out_ref[:, :HEAD] = attn_rows[:PAIR]
    out_ref[:, HEAD : 2 * HEAD] = attn_rows[PAIR:]
    scaled = share * SCALE
    query_grad = jnp.zeros((HEAD, width), jnp.float32)
    for step, unit in enumerate(unit_of):
        prob = score_ref[step * PAIR : (step + 1) * PAIR, :] * scaled
        change = (prob * (dot(others_ref[unit, :, HEAD:], grads, NT) - delta)).astype(jnp.bfloat16)
        query_grad = query_grad + dot(others_ref[unit, :, :HEAD], change, TN)
        given_ref[unit, :, :HEAD] = dot(change, queries, NN).astype(jnp.bfloat16)
    prob = score_ref[3 * PAIR :, :] * scaled
    grad_own = dot(own_ref[:, HEAD:], grads, NT)
    grad_far = dot(far_ref[:, HEAD:], grads, NT)
    change = prob * (jnp.where(near, grad_own, grad_far) - delta)
    change_own = jnp.where(near, change, 0.0).astype(jnp.bfloat16)
    change_far = jnp.where(near, 0.0, change).astype(jnp.bfloat16)
    query_grad = query_grad + dot(own_ref[:, :HEAD], change_own, TN)
    query_grad = query_grad + dot(far_ref[:, :HEAD], change_far, TN)
    kept_ref[:, :HEAD] = dot(change_own, queries, NN)
    back_ref[:, :HEAD] = dot(change_far, queries, NN)
    given_ref[here] = jnp.zeros((PAIR, 2 * HEAD), jnp.bfloat16)
    grad_rows = query_grad.T.astype(jnp.bfloat16)
    out_ref[:, 2 * HEAD : 3 * HEAD] = grad_rows[:PAIR]
    out_ref[:, 3 * HEAD :] = grad_rows[PAIR:]
    parts(out_ref, swap_ref, step_ref, skip_ref)


def parts(rows_ref, swap_ref, step_ref, skip_ref):
    member = lax.axis_index("yl")
    start = pl.multiple_of(jnp.where(member == 0, PAIR - SWAP, 0), 16)
    low = pl.multiple_of(jnp.where(member == 0, 0, PAIR - EDGE), 16)
    high = pl.multiple_of(jnp.where(member == 0, PAIR - EDGE, 0), 16)
    swap_ref[...] = rows_ref[pl.ds(start, SWAP), :]
    step_ref[...] = rows_ref[pl.ds(low, EDGE), :]
    skip_ref[...] = rows_ref[pl.ds(high, EDGE), :]


def gather_kernel(arrived_ref, kept_ref, back_ref, own_ref, send_ref):
    here = lax.axis_index("xh") * 2 + lax.axis_index("yh")
    own_ref[...] = kept_ref[...]
    send = back_ref[...]
    own = kept_ref[...]
    for unit in range(UNITS):
        part = arrived_ref[unit].astype(jnp.float32)
        own = own + jnp.where(unit > here, part, 0.0)
        send = send + jnp.where(unit < here, part, 0.0)
    own_ref[...] = own
    send_ref[...] = send.astype(jnp.bfloat16)


def total_kernel(own_ref, back_ref, out_ref, swap_ref, step_ref, skip_ref):
    out_ref[...] = (own_ref[...] + back_ref[...].astype(jnp.float32)).astype(jnp.bfloat16)
    parts(out_ref, swap_ref, step_ref, skip_ref)


def place_kernel(offsets_ref, rows_ref, swap_ref, step_ref, skip_ref, first_ref, second_ref):
    pair = pair_index()
    member = lax.axis_index("yl")
    start = offsets_ref[2 * pair + member]
    end = offsets_ref[2 * pair + member + 1]
    slot = lax.broadcasted_iota(jnp.int32, (SLOTS, 1), 0)
    place = slot + (start - pair * PAIR)
    inside = (place >= 0) & (place < PAIR)
    edge = place + jnp.where(member == 0, EDGE, -PAIR)
    live = slot < end - start
    mine = jnp.where(live, jnp.where(inside, place, PAIR + edge), -1)
    theirs = place - jnp.where(member == 0, 0, PAIR - SWAP)
    theirs = jnp.where(live, jnp.where(inside, theirs, SWAP + edge), -1)
    full = rows_ref.shape[1]
    width = full // 2
    pad = jnp.zeros((80, full), jnp.bfloat16)
    own = picked(SLOTS, mine, jnp.concatenate([rows_ref[...], skip_ref[...], pad], axis=0))
    other = picked(
        SLOTS, theirs, jnp.concatenate([swap_ref[...], step_ref[...], pad[:32]], axis=0)
    )

    @pl.when(member == 0)
    def _():
        first_ref[:, :width] = own[:, :width]
        first_ref[:, width:] = other[:, :width]
        second_ref[:, :width] = own[:, width:]
        second_ref[:, width:] = other[:, width:]

    @pl.when(member == 1)
    def _():
        first_ref[:, :width] = other[:, :width]
        first_ref[:, width:] = own[:, :width]
        second_ref[:, :width] = other[:, width:]
        second_ref[:, width:] = own[:, width:]


def placed(rows, swap, step, skip, offsets, name):
    blocks = range(2 * PAIRS)
    swap = lax.ppermute(swap, SEQ_AXES, [(j, j ^ 1) for j in blocks])
    step = lax.ppermute(
        step,
        SEQ_AXES,
        [(j, j + 2 * (j % 2) - 1) for j in blocks if 0 <= j + 2 * (j % 2) - 1 < 2 * PAIRS],
    )
    skip = lax.ppermute(
        skip,
        SEQ_AXES,
        [(j, j + 2 - 4 * (j % 2)) for j in blocks if 0 <= j + 2 - 4 * (j % 2) < 2 * PAIRS],
    )
    width = rows.shape[1]
    return call(
        place_kernel,
        [shape(SLOTS, width), shape(SLOTS, width)],
        [smem(), vmem(), vmem(), vmem(), vmem()],
        name=name,
    )(offsets, rows, swap, step, skip)


def on_device(q_old, k_old, value_old_layout, dout_old, old_offsets, new_offsets):
    pair_rows = pack(k_old, value_old_layout, "pack_keys")
    pair_rows = lax.all_to_all(pair_rows, GROUP_AXES, 0, 0, tiled=True)
    query_rows = pack(q_old, dout_old, "pack_queries")
    query_rows = lax.all_to_all(query_rows, GROUP_AXES, 0, 0, tiled=True)
    own = even_rows(pair_rows.reshape(2 * SLOTS, 2 * HEAD), old_offsets, "keys")
    far = lax.ppermute(own, "z", [(i, i + 1) for i in range(15)])
    chosen = call(choose_kernel, shape(UNITS, PAIR, 2 * HEAD), [vmem(), vmem()], name="choose")(own, far)
    others = lax.all_to_all(chosen, PLANE_AXES, 0, 0, tiled=True)
    rows = even_rows(query_rows.reshape(2 * SLOTS, 4 * HEAD), old_offsets, "queries")
    wide = 4 * HEAD
    results, swap, step, skip, given, kept, back = call(
        attend_kernel,
        [
            shape(PAIR, wide),
            shape(SWAP, wide),
            shape(EDGE, wide),
            shape(EDGE, wide),
            shape(UNITS, PAIR, 2 * HEAD),
            shape(PAIR, 2 * HEAD, dtype=jnp.float32),
            shape(PAIR, 2 * HEAD, dtype=jnp.float32),
        ],
        [vmem(), vmem(), vmem(), vmem()],
        [pltpu.VMEM((UNITS * PAIR, 2 * PAIR), jnp.float32)],
        name="attend",
        flops=10**9,
    )(rows, own, far, others)
    arrived = lax.all_to_all(given, PLANE_AXES, 0, 0, tiled=True)
    own_grad, send = call(
        gather_kernel,
        [shape(PAIR, 2 * HEAD, dtype=jnp.float32), shape(PAIR, 2 * HEAD)],
        [vmem(), vmem(), vmem()],
        name="gather",
    )(arrived, kept, back)
    returned = lax.ppermute(send, "z", [(i + 1, i) for i in range(15)])
    attn_out, grad_query_out = placed(results, swap, step, skip, new_offsets, "place_rows")
    narrow = 2 * HEAD
    pair_grads = call(
        total_kernel,
        [shape(PAIR, narrow), shape(SWAP, narrow), shape(EDGE, narrow), shape(EDGE, narrow)],
        [vmem(), vmem()],
        name="total",
    )(own_grad, returned)
    grad_key_out, grad_value_out = placed(*pair_grads, new_offsets, "place_grads")
    return attn_out, grad_query_out, grad_key_out, grad_value_out


def solution(mesh):
    cut = Mesh(mesh.devices.reshape(16, 2, 2, 2, 2, 2), AXES)
    rows = P(AXES, None)
    return jax.shard_map(
        on_device,
        mesh=cut,
        in_specs=(rows, rows, rows, rows, P(), P()),
        out_specs=(P(SEQ_AXES, ("xl", "c")),) * 4,
        check_vma=False,
    )
```

```python
import jax
import jax.numpy as jnp
from jax import lax
from jax.experimental import pallas as pl
from jax.experimental.pallas import tpu as pltpu
from jax.sharding import Mesh, PartitionSpec as P

PAIR = 256
SLOTS = 224
EDGE = 48
HEAD = 128
UNITS = 4
PAIRS = 64
SWAP = PAIR - 80
SCALE = 168.0 ** (-0.5)
LOG2E = 1.4426950408889634
OUTSIDE = -1e30

AXES = ("z", "xh", "yh", "yl", "xl", "c")
PAIR_AXES = ("z", "xh", "yh")
SEQ_AXES = ("z", "xh", "yh", "yl")
GROUP_AXES = ("yl", "xl", "c")

NT = (((1,), (1,)), ((), ()))
NN = (((1,), (0,)), ((), ()))
TN = (((0,), (0,)), ((), ()))


def dot(a, b, dims):
    return lax.dot_general(a, b, dims, preferred_element_type=jnp.float32)


def pair_index():
    return (lax.axis_index("z") * 2 + lax.axis_index("xh")) * 2 + lax.axis_index("yh")


def vmem():
    return pl.BlockSpec(memory_space=pltpu.VMEM)


def smem():
    return pl.BlockSpec(memory_space=pltpu.SMEM)


def call(kernel, outs, specs, scratch=(), name=None, flops=0, limit=4):
    many = isinstance(outs, (list, tuple))
    return pl.pallas_call(
        kernel,
        out_shape=outs,
        in_specs=specs,
        out_specs=[vmem() for _ in outs] if many else vmem(),
        scratch_shapes=list(scratch),
        name=name,
        compiler_params=pltpu.CompilerParams(vmem_limit_bytes=limit << 20),
        cost_estimate=pl.CostEstimate(flops=flops, bytes_accessed=1 << 20, transcendentals=0),
    )


def shape(*dims, dtype=jnp.bfloat16):
    return jax.ShapeDtypeStruct(dims, dtype)


def picked(rows, source, candidates):
    count = candidates.shape[0]
    columns = lax.broadcasted_iota(jnp.int32, (rows, count), 1)
    chosen = (columns == source).astype(jnp.float32).astype(jnp.bfloat16)
    return dot(chosen, candidates, NN).astype(jnp.bfloat16)


def pack_kernel(keys_ref, values_ref, queries_ref, grads_ref, out_ref):
    for target in range(8):
        head = (target % 4) * 2 + target // 4
        start = 0
        for ref in (keys_ref, values_ref, queries_ref, grads_ref):
            width = ref.shape[1] // 8
            out_ref[target, :, start : start + width] = ref[:, head * width : (head + 1) * width]
            start += width


def edges_kernel(offsets_ref, slots_ref, left_ref, right_ref):
    pair = pair_index()
    first = offsets_ref[2 * pair]
    middle = offsets_ref[2 * pair + 1]
    row = lax.broadcasted_iota(jnp.int32, (2 * EDGE, 1), 0)
    to_left = row + (pair * PAIR - EDGE - first)
    to_right = row + (SLOTS - EDGE + (pair + 1) * PAIR - middle)
    source = jnp.where(row < EDGE, to_left, to_right)
    both = picked(2 * EDGE, source, slots_ref[...])
    left_ref[...] = both[:EDGE]
    right_ref[...] = both[EDGE:]


def even_kernel(offsets_ref, slots_ref, left_ref, right_ref, keys_ref, rows_ref):
    pair = pair_index()
    first = offsets_ref[2 * pair]
    middle = offsets_ref[2 * pair + 1]
    last = offsets_ref[2 * pair + 2]
    row = lax.broadcasted_iota(jnp.int32, (PAIR, 1), 0)
    place = row + pair * PAIR
    source = jnp.where(
        place < first,
        2 * SLOTS + row,
        jnp.where(
            place < middle,
            place - first,
            jnp.where(place < last, SLOTS + place - middle, 2 * SLOTS + 2 * EDGE - PAIR + row),
        ),
    )
    width = slots_ref.shape[1]
    candidates = jnp.concatenate(
        [slots_ref[...], left_ref[...], right_ref[...], jnp.zeros((96, width), jnp.bfloat16)], axis=0
    )
    rows = picked(PAIR, source, candidates)
    keys_ref[...] = rows[:, : 2 * HEAD]
    rows_ref[...] = rows[:, 2 * HEAD :]


def shifted(value, steps):
    pairs = range(max(0, -steps), min(PAIRS, PAIRS - steps))
    return lax.ppermute(value, PAIR_AXES, [(i, i + steps) for i in pairs])


def even_rows(slots, offsets):
    width = slots.shape[1]
    left, right = call(
        edges_kernel, [shape(EDGE, width), shape(EDGE, width)], [smem(), vmem()], name="edges"
    )(offsets, slots)
    return call(
        even_kernel,
        [shape(PAIR, 2 * HEAD), shape(PAIR, 4 * HEAD)],
        [smem(), vmem(), vmem(), vmem()],
        name="even",
    )(offsets, slots, shifted(right, 1), shifted(left, -1))


def attend_kernel(
    rows_ref, own_ref, first_ref, second_ref, third_ref, far_ref,
    out_ref, kept_ref, given1_ref, given2_ref, given3_ref, back_ref, score_ref,
):
    pair = pair_index()
    others = (first_ref, second_ref, third_ref)
    given = (given1_ref, given2_ref, given3_ref)
    width = 2 * PAIR
    queries = jnp.concatenate([rows_ref[:, :HEAD], rows_ref[:, HEAD : 2 * HEAD]], axis=0)
    grads = jnp.concatenate([rows_ref[:, 2 * HEAD : 3 * HEAD], rows_ref[:, 3 * HEAD :]], axis=0)
    key_row = lax.broadcasted_iota(jnp.int32, (PAIR, width), 0)
    query_row = lax.broadcasted_iota(jnp.int32, (PAIR, width), 1) & (PAIR - 1)
    near = key_row <= query_row
    top = jnp.full((1, width), OUTSIDE, jnp.float32)
    for step, ref in enumerate(others):
        bias = jnp.where(pair > step, 0.0, OUTSIDE)
        score = dot(ref[:, :HEAD], queries, NT) * (SCALE * LOG2E) + bias
        score_ref[step * PAIR : (step + 1) * PAIR, :] = score
        top = jnp.maximum(top, jnp.max(score, axis=0, keepdims=True))
    bias = jnp.where(pair >= UNITS, 0.0, OUTSIDE)
    score = jnp.where(
        near,
        dot(own_ref[:, :HEAD], queries, NT) * (SCALE * LOG2E),
        dot(far_ref[:, :HEAD], queries, NT) * (SCALE * LOG2E) + bias,
    )
    score_ref[3 * PAIR :, :] = score
    top = jnp.maximum(top, jnp.max(score, axis=0, keepdims=True))
    total = jnp.zeros((1, width), jnp.float32)
    for step in range(UNITS):
        weight = jnp.exp2(score_ref[step * PAIR : (step + 1) * PAIR, :] - top)
        score_ref[step * PAIR : (step + 1) * PAIR, :] = weight
        total = total + jnp.sum(weight, axis=0, keepdims=True)
    share = 1.0 / total
    zero = jnp.zeros((), jnp.bfloat16)
    attn = jnp.zeros((HEAD, width), jnp.float32)
    for step, ref in enumerate(others):
        prob = (score_ref[step * PAIR : (step + 1) * PAIR, :] * share).astype(jnp.bfloat16)
        attn = attn + dot(ref[:, HEAD:], prob, TN)
        given[step][:, HEAD:] = dot(prob, grads, NN).astype(jnp.bfloat16)
    prob = score_ref[3 * PAIR :, :] * share
    prob_own = jnp.where(near, prob, 0.0).astype(jnp.bfloat16)
    prob_far = jnp.where(near, 0.0, prob).astype(jnp.bfloat16)
    attn = attn + dot(own_ref[:, HEAD:], prob_own, TN) + dot(far_ref[:, HEAD:], prob_far, TN)
    kept_ref[:, HEAD:] = dot(prob_own, grads, NN)
    back_ref[:, HEAD:] = dot(prob_far, grads, NN).astype(jnp.bfloat16)
    attn = attn.astype(jnp.bfloat16).astype(jnp.float32)
    grads_t = grads.astype(jnp.float32).T
    delta = jnp.sum(attn * grads_t, axis=0, keepdims=True)
    attn_rows = attn.T.astype(jnp.bfloat16)
    out_ref[:, :HEAD] = attn_rows[:PAIR]
    out_ref[:, HEAD : 2 * HEAD] = attn_rows[PAIR:]
    scaled = share * SCALE
    query_grad = jnp.zeros((HEAD, width), jnp.float32)
    for step, ref in enumerate(others):
        prob = score_ref[step * PAIR : (step + 1) * PAIR, :] * scaled
        change = (prob * (dot(ref[:, HEAD:], grads, NT) - delta)).astype(jnp.bfloat16)
        query_grad = query_grad + dot(ref[:, :HEAD], change, TN)
        given[step][:, :HEAD] = dot(change, queries, NN).astype(jnp.bfloat16)
    prob = score_ref[3 * PAIR :, :] * scaled
    grad_own = dot(own_ref[:, HEAD:], grads, NT)
    grad_far = dot(far_ref[:, HEAD:], grads, NT)
    change = prob * (jnp.where(near, grad_own, grad_far) - delta)
    change_own = jnp.where(near, change, 0.0).astype(jnp.bfloat16)
    change_far = jnp.where(near, 0.0, change).astype(jnp.bfloat16)
    query_grad = query_grad + dot(own_ref[:, :HEAD], change_own, TN)
    query_grad = query_grad + dot(far_ref[:, :HEAD], change_far, TN)
    kept_ref[:, :HEAD] = dot(change_own, queries, NN)
    back_ref[:, :HEAD] = dot(change_far, queries, NN).astype(jnp.bfloat16)
    grad_rows = query_grad.T.astype(jnp.bfloat16)
    out_ref[:, 2 * HEAD : 3 * HEAD] = grad_rows[:PAIR]
    out_ref[:, 3 * HEAD :] = grad_rows[PAIR:]


def parts(rows_ref, swap_ref, step_ref, skip_ref):
    member = lax.axis_index("yl")
    start = pl.multiple_of(jnp.where(member == 0, PAIR - SWAP, 0), 16)
    low = pl.multiple_of(jnp.where(member == 0, 0, PAIR - EDGE), 16)
    high = pl.multiple_of(jnp.where(member == 0, PAIR - EDGE, 0), 16)
    swap_ref[...] = rows_ref[pl.ds(start, SWAP), :]
    step_ref[...] = rows_ref[pl.ds(low, EDGE), :]
    skip_ref[...] = rows_ref[pl.ds(high, EDGE), :]


def total_kernel(rows_ref, own_ref, back1_ref, back2_ref, back3_ref, back4_ref, out_ref, swap_ref, step_ref, skip_ref):
    total = own_ref[...]
    for ref in (back1_ref, back2_ref, back3_ref, back4_ref):
        total = total + ref[...].astype(jnp.float32)
    out_ref[:, : 4 * HEAD] = rows_ref[...]
    out_ref[:, 4 * HEAD :] = total.astype(jnp.bfloat16)
    parts(out_ref, swap_ref, step_ref, skip_ref)


def place_kernel(offsets_ref, rows_ref, swap_ref, step_ref, skip_ref, *out_refs):
    pair = pair_index()
    member = lax.axis_index("yl")
    start = offsets_ref[2 * pair + member]
    end = offsets_ref[2 * pair + member + 1]
    slot = lax.broadcasted_iota(jnp.int32, (SLOTS, 1), 0)
    place = slot + (start - pair * PAIR)
    inside = (place >= 0) & (place < PAIR)
    edge = place + jnp.where(member == 0, EDGE, -PAIR)
    live = slot < end - start
    mine = jnp.where(live, jnp.where(inside, place, PAIR + edge), -1)
    theirs = place - jnp.where(member == 0, 0, PAIR - SWAP)
    theirs = jnp.where(live, jnp.where(inside, theirs, SWAP + edge), -1)
    pad = jnp.zeros((80, rows_ref.shape[1]), jnp.bfloat16)
    own = picked(SLOTS, mine, jnp.concatenate([rows_ref[...], skip_ref[...], pad], axis=0))
    other = picked(
        SLOTS, theirs, jnp.concatenate([swap_ref[...], step_ref[...], pad[:32]], axis=0)
    )

    def store(low, high):
        column = 0
        for ref in out_refs:
            width = ref.shape[1] // 2
            ref[:, :width] = low[:, column : column + width]
            ref[:, width:] = high[:, column : column + width]
            column += width

    @pl.when(member == 0)
    def _():
        store(own, other)

    @pl.when(member == 1)
    def _():
        store(other, own)


def placed(rows, swap, step, skip, offsets):
    blocks = range(2 * PAIRS)
    swap = lax.ppermute(swap, SEQ_AXES, [(j, j ^ 1) for j in blocks])
    step = lax.ppermute(
        step,
        SEQ_AXES,
        [(j, j + 2 * (j % 2) - 1) for j in blocks if 0 <= j + 2 * (j % 2) - 1 < 2 * PAIRS],
    )
    skip = lax.ppermute(
        skip,
        SEQ_AXES,
        [(j, j + 2 - 4 * (j % 2)) for j in blocks if 0 <= j + 2 - 4 * (j % 2) < 2 * PAIRS],
    )
    return call(
        place_kernel,
        [shape(SLOTS, 4 * HEAD)] * 2 + [shape(SLOTS, 2 * HEAD)] * 2,
        [smem(), vmem(), vmem(), vmem(), vmem()],
        name="place",
        limit=6,
    )(offsets, rows, swap, step, skip)


def on_device(q_old, k_old, value_old_layout, dout_old, old_offsets, new_offsets):
    packed = call(pack_kernel, shape(8, 56, 6 * HEAD), [vmem()] * 4, name="pack")(
        k_old, value_old_layout, q_old, dout_old
    )
    slots = lax.all_to_all(packed, GROUP_AXES, 0, 0, tiled=True)
    own, rows = even_rows(slots.reshape(2 * SLOTS, 6 * HEAD), old_offsets)
    others = [shifted(own, step + 1) for step in range(UNITS)]
    wide, narrow = 4 * HEAD, 2 * HEAD
    results, kept, *given = call(
        attend_kernel,
        [shape(PAIR, wide), shape(PAIR, narrow, dtype=jnp.float32)] + [shape(PAIR, narrow)] * UNITS,
        [vmem()] * 6,
        [pltpu.VMEM((UNITS * PAIR, 2 * PAIR), jnp.float32)],
        name="attend",
        flops=10**9,
        limit=24,
    )(rows, own, *others)
    back = [shifted(value, -step - 1) for step, value in enumerate(given)]
    full = wide + narrow
    parts_of = call(
        total_kernel,
        [shape(PAIR, full), shape(SWAP, full), shape(EDGE, full), shape(EDGE, full)],
        [vmem()] * 6,
        name="total",
    )(results, kept, *back)
    return tuple(placed(*parts_of, new_offsets))


def solution(mesh):
    cut = Mesh(mesh.devices.reshape(16, 2, 2, 2, 2, 2), AXES)
    rows = P(AXES, None)
    return jax.shard_map(
        on_device,
        mesh=cut,
        in_specs=(rows, rows, rows, rows, P(), P()),
        out_specs=(P(SEQ_AXES, ("xl", "c")),) * 4,
        check_vma=False,
    )
```

```python
import jax
import jax.numpy as jnp
from jax import lax
from jax.experimental import pallas as pl
from jax.experimental.pallas import tpu as pltpu
from jax.sharding import Mesh, PartitionSpec as P


PAIR = 256
SLOTS = 224
LEAD = 48
EDGE = 96
SPAN = PAIR + EDGE
HEAD = 128
UNITS = 4
PAIRS = 64
SCALE = 168.0 ** (-0.5)
LOG2E = 1.4426950408889634
OUTSIDE = -1e30

AXES = ("z", "xh", "yh", "yl", "xl", "c")
SEQ_AXES = ("z", "xh", "yh", "yl")
GROUP_AXES = ("yl", "xl", "c")

NT = (((1,), (1,)), ((), ()))
NN = (((1,), (0,)), ((), ()))
TN = (((0,), (0,)), ((), ()))


def dot(a, b, dims):
    return lax.dot_general(a, b, dims, preferred_element_type=jnp.float32)


def pair_index():
    return (lax.axis_index("z") * 2 + lax.axis_index("xh")) * 2 + lax.axis_index("yh")


def vmem():
    return pl.BlockSpec(memory_space=pltpu.VMEM)


def call(kernel, outs, specs, scratch=(), flops=0, limit=4):
    many = isinstance(outs, (list, tuple))
    return pl.pallas_call(
        kernel,
        out_shape=outs,
        in_specs=specs,
        out_specs=[vmem() for _ in outs] if many else vmem(),
        scratch_shapes=list(scratch),
        compiler_params=pltpu.CompilerParams(vmem_limit_bytes=limit << 20),
        cost_estimate=pl.CostEstimate(flops=flops, bytes_accessed=1 << 20, transcendentals=0),
    )


def shape(*dims, dtype=jnp.bfloat16):
    return jax.ShapeDtypeStruct(dims, dtype)


def picked(rows, source, candidates):
    count = candidates.shape[0]
    columns = lax.broadcasted_iota(jnp.int32, (rows, count), 1)
    chosen = (columns == source).astype(jnp.float32).astype(jnp.bfloat16)
    return dot(chosen, candidates, NN).astype(jnp.bfloat16)


def compute_member():
    return lax.axis_index("yl") ^ lax.axis_index("yh")


def pack_kernel(
    keys_ref, values_ref, queries_ref, grads_ref, old_ref, new_ref, out_ref, facts_ref,
    offsets_ref, sems, offset_sems,
):
    old_copy = pltpu.make_async_copy(old_ref, offsets_ref.at[0], offset_sems.at[0])
    new_copy = pltpu.make_async_copy(new_ref, offsets_ref.at[1], offset_sems.at[1])
    old_copy.start()
    new_copy.start()
    mirrored = lax.axis_index("yh")
    copies = []
    for target in range(8):
        head = (target % 4) * 2 + ((target // 4) ^ mirrored)
        begin = 0
        for ref in (keys_ref, values_ref, queries_ref, grads_ref):
            width = ref.shape[1] // 8
            source = ref.at[:, pl.ds(pl.multiple_of(head * width, HEAD), width)]
            copy = pltpu.make_async_copy(
                source, out_ref.at[target, :, pl.ds(begin, width)], sems.at[len(copies)]
            )
            copy.start()
            copies.append(copy)
            begin += width
    old_copy.wait()
    new_copy.wait()
    pair = pair_index()
    block = 2 * pair + lax.axis_index("yl")
    facts = (
        offsets_ref[0, 2 * pair],
        offsets_ref[0, 2 * pair + 1],
        offsets_ref[0, 2 * pair + 2],
        offsets_ref[1, block],
        offsets_ref[1, block + 1],
    )
    for row, fact in enumerate(facts):
        facts_ref[row : row + 1, :] = jnp.full((1, HEAD), fact, jnp.int32)
    facts_ref[len(facts) :, :] = jnp.zeros((8 - len(facts), HEAD), jnp.int32)
    for copy in copies:
        copy.wait()


def raw_kernel(facts_ref, slots_ref, first_ref, edge_ref, rows_ref):
    start = pair_index() * PAIR - LEAD
    place = lax.broadcasted_iota(jnp.int32, (SPAN, 1), 0) + start
    first = facts_ref[0:1, 0:1]
    middle = facts_ref[1:2, 0:1]
    last = facts_ref[2:3, 0:1]
    source = jnp.where(place < middle, place - first, SLOTS + place - middle)
    source = jnp.where((place >= first) & (place < last), source, -1)
    rows = picked(SPAN, source, slots_ref[...])
    first_ref[...] = rows[:, : 2 * HEAD]
    edge_ref[...] = rows[PAIR:, 2 * HEAD :]
    rows_ref[...] = rows[:PAIR, 2 * HEAD :]


def joined(rows, edge):
    return jnp.concatenate([rows[:EDGE] + edge, rows[EDGE:]], axis=0)


def relay_kernel(mine_ref, first_ref, second_ref, fourth_ref):
    whole = joined(mine_ref[:PAIR], first_ref[PAIR:SPAN])
    edge = mine_ref[PAIR:SPAN]
    second_ref[:PAIR] = whole
    second_ref[PAIR:SPAN] = edge
    second_ref[SPAN:] = first_ref[:PAIR]
    fourth_ref[:PAIR] = whole
    fourth_ref[PAIR:] = edge


def attend_kernel(
    rows_ref, edge_ref, mine_ref, first_ref, second_ref, fourth_ref,
    out_ref, edge_out_ref, kept_ref, near_ref, give2_ref, give4_ref, score_ref,
):
    start = pair_index() * PAIR - LEAD
    width = 2 * PAIR
    own = mine_ref[:PAIR]
    far = fourth_ref[:PAIR]
    others = (
        joined(first_ref[:PAIR], second_ref[PAIR:SPAN]),
        second_ref[:PAIR],
        joined(second_ref[SPAN:], fourth_ref[PAIR:]),
    )

    def stacked(column):
        parts = []
        for head in range(2):
            columns = slice(column + head * HEAD, column + (head + 1) * HEAD)
            parts.append(joined(rows_ref[:, columns], edge_ref[:, columns]))
        return jnp.concatenate(parts, axis=0)

    queries = stacked(0)
    grads = stacked(2 * HEAD)
    key_row = lax.broadcasted_iota(jnp.int32, (PAIR, width), 0)
    query_row = lax.broadcasted_iota(jnp.int32, (PAIR, width), 1) & (PAIR - 1)
    near = key_row <= query_row
    column = lax.broadcasted_iota(jnp.int32, (1, width), 1) & (PAIR - 1)
    positive = (column + start >= 0).astype(jnp.float32)
    place = lax.broadcasted_iota(jnp.int32, (PAIR, 1), 0) + start

    def scores(keys, distance):
        bias = jnp.where(place - distance * PAIR >= 0, 0.0, OUTSIDE)
        return dot(keys[:, :HEAD], queries, NT) * (SCALE * LOG2E) + bias * positive

    top = jnp.full((1, width), OUTSIDE, jnp.float32)
    for step, keys in enumerate(others):
        score = scores(keys, step + 1)
        score_ref[step * PAIR : (step + 1) * PAIR, :] = score
        top = jnp.maximum(top, jnp.max(score, axis=0, keepdims=True))
    score = jnp.where(near, scores(own, 0), scores(far, UNITS))
    score_ref[3 * PAIR :, :] = score
    top = jnp.maximum(top, jnp.max(score, axis=0, keepdims=True))
    total = jnp.zeros((1, width), jnp.float32)
    for step in range(UNITS):
        weight = jnp.exp2(score_ref[step * PAIR : (step + 1) * PAIR, :] - top)
        score_ref[step * PAIR : (step + 1) * PAIR, :] = weight
        total = total + jnp.sum(weight, axis=0, keepdims=True)
    share = 1.0 / total

    def keep(step, columns, value):
        rounded = value.astype(jnp.bfloat16)
        if step == 0:
            kept_ref[:, columns] = value
        elif step == 1:
            near_ref[:, columns] = value
            give2_ref[PAIR:SPAN, columns] = rounded[:EDGE]
        elif step == 2:
            give2_ref[:PAIR, columns] = rounded
        elif step == 3:
            give2_ref[SPAN:, columns] = rounded
            give4_ref[PAIR:, columns] = rounded[:EDGE]
        else:
            give4_ref[:PAIR, columns] = rounded

    key_columns = slice(0, HEAD)
    value_columns = slice(HEAD, 2 * HEAD)
    attn = jnp.zeros((HEAD, width), jnp.float32)
    for step, keys in enumerate(others):
        prob = (score_ref[step * PAIR : (step + 1) * PAIR, :] * share).astype(jnp.bfloat16)
        attn = attn + dot(keys[:, HEAD:], prob, TN)
        keep(step + 1, value_columns, dot(prob, grads, NN))
    prob = score_ref[3 * PAIR :, :] * share
    prob_own = jnp.where(near, prob, 0.0).astype(jnp.bfloat16)
    prob_far = jnp.where(near, 0.0, prob).astype(jnp.bfloat16)
    attn = attn + dot(own[:, HEAD:], prob_own, TN) + dot(far[:, HEAD:], prob_far, TN)
    keep(0, value_columns, dot(prob_own, grads, NN))
    keep(UNITS, value_columns, dot(prob_far, grads, NN))
    attn = attn.astype(jnp.bfloat16).astype(jnp.float32)
    delta = jnp.sum(attn * grads.astype(jnp.float32).T, axis=0, keepdims=True)
    attn_rows = attn.T.astype(jnp.bfloat16)
    out_ref[:, :HEAD] = attn_rows[:PAIR]
    out_ref[:, HEAD : 2 * HEAD] = attn_rows[PAIR:]
    scaled = share * SCALE
    query_grad = jnp.zeros((HEAD, width), jnp.float32)
    for step, keys in enumerate(others):
        prob = score_ref[step * PAIR : (step + 1) * PAIR, :] * scaled
        change = (prob * (dot(keys[:, HEAD:], grads, NT) - delta)).astype(jnp.bfloat16)
        query_grad = query_grad + dot(keys[:, :HEAD], change, TN)
        keep(step + 1, key_columns, dot(change, queries, NN))
    prob = score_ref[3 * PAIR :, :] * scaled
    grad_prob = jnp.where(near, dot(own[:, HEAD:], grads, NT), dot(far[:, HEAD:], grads, NT))
    change = prob * (grad_prob - delta)
    change_own = jnp.where(near, change, 0.0).astype(jnp.bfloat16)
    change_far = jnp.where(near, 0.0, change).astype(jnp.bfloat16)
    query_grad = query_grad + dot(own[:, :HEAD], change_own, TN)
    query_grad = query_grad + dot(far[:, :HEAD], change_far, TN)
    keep(0, key_columns, dot(change_own, queries, NN))
    keep(UNITS, key_columns, dot(change_far, queries, NN))
    grad_rows = query_grad.T.astype(jnp.bfloat16)
    out_ref[:, 2 * HEAD : 3 * HEAD] = grad_rows[:PAIR]
    out_ref[:, 3 * HEAD :] = grad_rows[PAIR:]
    edge_out_ref[...] = out_ref[:EDGE, :]


def merge_kernel(kept_ref, near_ref, back2_ref, back4_ref, sum_ref, give_ref):
    def read(ref, start, rows):
        return ref[start : start + rows].astype(jnp.float32)

    sum_ref[:PAIR] = kept_ref[...] + read(back2_ref, 0, PAIR) + read(back4_ref, 0, PAIR)
    sum_ref[PAIR:] = read(back2_ref, PAIR, EDGE) + read(back4_ref, PAIR, EDGE)
    give_ref[:PAIR] = (near_ref[...] + read(back2_ref, SPAN, PAIR)).astype(jnp.bfloat16)
    edge = kept_ref[:EDGE] + read(back2_ref, 0, EDGE) + read(back4_ref, 0, EDGE)
    give_ref[PAIR:] = edge.astype(jnp.bfloat16)


def swap_rows(out_ref, swap_ref):
    start = pl.multiple_of(jnp.where(lax.axis_index("yl") == 0, SPAN - SLOTS, 0), 16)
    swap_ref[...] = out_ref[pl.ds(start, SLOTS), :]


def span_kernel(rows_ref, edge_ref, out_ref, swap_ref):
    out_ref[:PAIR] = rows_ref[...]
    out_ref[PAIR:] = edge_ref[...]
    swap_rows(out_ref, swap_ref)


def total_kernel(sum_ref, back_ref, out_ref, swap_ref):
    out_ref[...] = (sum_ref[...] + back_ref[...].astype(jnp.float32)).astype(jnp.bfloat16)
    swap_rows(out_ref, swap_ref)


def place_kernel(facts_ref, rows_ref, swap_ref, first_ref, second_ref):
    start = facts_ref[3:4, 0:1]
    end = facts_ref[4:5, 0:1]
    slot = lax.broadcasted_iota(jnp.int32, (SLOTS, 1), 0)
    place = slot + (start - (pair_index() * PAIR - LEAD))
    live = slot < end - start
    partner_start = jnp.where(lax.axis_index("yl") == 0, 0, SPAN - SLOTS)
    own = picked(SLOTS, jnp.where(live, place, -1), rows_ref[...])
    other = picked(SLOTS, jnp.where(live, place - partner_start, -1), swap_ref[...])
    width = first_ref.shape[1] // 2

    def store(low, high):
        first_ref[:, :width] = low[:, :width]
        first_ref[:, width:] = high[:, :width]
        second_ref[:, :width] = low[:, width:]
        second_ref[:, width:] = high[:, width:]

    @pl.when(compute_member() == 0)
    def _():
        store(own, other)

    @pl.when(compute_member() == 1)
    def _():
        store(other, own)


def placed(facts, rows, swapped):
    width = rows.shape[1]
    return call(place_kernel, [shape(SLOTS, width)] * 2, [vmem()] * 3)(facts, rows, swapped)


def swapped(value):
    return lax.ppermute(value, "yl", [(0, 1), (1, 0)])


def shifted(value, steps):
    route = [
        (2 * pair + member, 2 * ((pair + steps) % PAIRS) + (member ^ (steps & 1)))
        for pair in range(PAIRS)
        for member in range(2)
    ]
    return lax.ppermute(value, SEQ_AXES, route)


def layer(q_old, k_old, value_old_layout, dout_old, old_offsets, new_offsets):
    wide, narrow, full = 4 * HEAD, 2 * HEAD, 6 * HEAD
    packed, facts = call(
        pack_kernel,
        [shape(8, 56, full), shape(8, HEAD, dtype=jnp.int32)],
        [pl.BlockSpec(memory_space=pltpu.HBM)] * 6,
        [
            pltpu.SMEM((2, old_offsets.shape[0]), jnp.int32),
            pltpu.SemaphoreType.DMA((32,)),
            pltpu.SemaphoreType.DMA((2,)),
        ],
        limit=60,
    )(k_old, value_old_layout, q_old, dout_old, old_offsets, new_offsets)
    slots = lax.all_to_all(packed, GROUP_AXES, 0, 0, tiled=True).reshape(2 * SLOTS, full)
    first, edge, rows = call(
        raw_kernel, [shape(SPAN, narrow), shape(EDGE, wide), shape(PAIR, wide)], [vmem()] * 2
    )(facts, slots)
    from_first = shifted(first, 1)
    from_edge = shifted(edge, 1)
    second, fourth = call(
        relay_kernel, [shape(SPAN + PAIR, narrow), shape(SPAN, narrow)], [vmem()] * 2
    )(first, from_first)
    from_second = shifted(second, 2)
    from_fourth = shifted(fourth, 4)
    results, result_edge, kept, near, give2, give4 = call(
        attend_kernel,
        [
            shape(PAIR, wide),
            shape(EDGE, wide),
            shape(PAIR, narrow, dtype=jnp.float32),
            shape(PAIR, narrow, dtype=jnp.float32),
            shape(SPAN + PAIR, narrow),
            shape(SPAN, narrow),
        ],
        [vmem()] * 6,
        [pltpu.VMEM((UNITS * PAIR, 2 * PAIR), jnp.float32)],
        flops=10**9,
        limit=24,
    )(rows, from_edge, second, from_first, from_second, from_fourth)
    back2 = shifted(give2, -2)
    back4 = shifted(give4, -4)
    back_edge = shifted(result_edge, -1)
    sums, give = call(
        merge_kernel, [shape(SPAN, narrow, dtype=jnp.float32), shape(SPAN, narrow)], [vmem()] * 4
    )(kept, near, back2, back4)
    back = shifted(give, -1)
    span_rows, row_swap = call(
        span_kernel, [shape(SPAN, wide), shape(SLOTS, wide)], [vmem()] * 2
    )(results, back_edge)
    other_rows = swapped(row_swap)
    totals, total_swap = call(
        total_kernel, [shape(SPAN, narrow), shape(SLOTS, narrow)], [vmem()] * 2
    )(sums, back)
    other_totals = swapped(total_swap)
    attn_out, grad_query_out = placed(facts, span_rows, other_rows)
    grad_key_out, grad_value_out = placed(facts, totals, other_totals)
    return attn_out, grad_query_out, grad_key_out, grad_value_out


def solution(mesh):
    cut = Mesh(mesh.devices.reshape(16, 2, 2, 2, 2, 2), AXES)
    rows = P(AXES, None)
    return jax.shard_map(
        layer,
        mesh=cut,
        in_specs=(rows, rows, rows, rows, P(), P()),
        out_specs=(P(SEQ_AXES, ("xl", "c")),) * 4,
        check_vma=False,
    )
```

```python
import jax
import jax.numpy as jnp
from jax import lax
from jax.experimental import pallas as pl
from jax.experimental.pallas import tpu as pltpu
from jax.sharding import Mesh, PartitionSpec as P


PAIR = 256
SLOTS = 224
LEAD = 48
EXTRA = 64
EDGE = 96
SPAN = PAIR + EDGE
HEAD = 128
UNITS = 4
PAIRS = 64
SCALE = 168.0 ** (-0.5)
LOG2E = 1.4426950408889634
OUTSIDE = -1e30

AXES = ("z", "xh", "yh", "yl", "xl", "c")
SEQ_AXES = ("z", "xh", "yh", "yl")
GROUP_AXES = ("yl", "xl", "c")

NT = (((1,), (1,)), ((), ()))
NN = (((1,), (0,)), ((), ()))
TN = (((0,), (0,)), ((), ()))


def dot(a, b, dims):
    return lax.dot_general(a, b, dims, preferred_element_type=jnp.float32)


def pair_index():
    return (lax.axis_index("z") * 2 + lax.axis_index("xh")) * 2 + lax.axis_index("yh")


def vmem():
    return pl.BlockSpec(memory_space=pltpu.VMEM)


def call(kernel, outs, specs, scratch=(), flops=0, limit=4):
    many = isinstance(outs, (list, tuple))
    return pl.pallas_call(
        kernel,
        out_shape=outs,
        in_specs=specs,
        out_specs=[vmem() for _ in outs] if many else vmem(),
        scratch_shapes=list(scratch),
        compiler_params=pltpu.CompilerParams(vmem_limit_bytes=limit << 20),
        cost_estimate=pl.CostEstimate(flops=flops, bytes_accessed=1 << 20, transcendentals=0),
    )


def shape(*dims, dtype=jnp.bfloat16):
    return jax.ShapeDtypeStruct(dims, dtype)


def picked(rows, source, candidates):
    count = candidates.shape[0]
    columns = lax.broadcasted_iota(jnp.int32, (rows, count), 1)
    chosen = (columns == source).astype(jnp.float32).astype(jnp.bfloat16)
    return dot(chosen, candidates, NN).astype(jnp.bfloat16)


def compute_member():
    return lax.axis_index("yl") ^ lax.axis_index("yh")


def start_packing(refs, out_ref, sems):
    mirrored = lax.axis_index("yh")
    copies = []
    for target in range(8):
        head = (target % 4) * 2 + ((target // 4) ^ mirrored)
        begin = 0
        for ref in refs:
            width = ref.shape[1] // 8
            source = ref.at[:, pl.ds(pl.multiple_of(head * width, HEAD), width)]
            copy = pltpu.make_async_copy(
                source, out_ref.at[target, :, pl.ds(begin, width)], sems.at[len(copies)]
            )
            copy.start()
            copies.append(copy)
            begin += width
    return copies


def pack_kernel(first_ref, second_ref, out_ref, sems):
    for copy in start_packing((first_ref, second_ref), out_ref, sems):
        copy.wait()


def facts_kernel(old_ref, new_ref, facts_ref, offsets_ref, sems):
    copies = [
        pltpu.make_async_copy(ref, offsets_ref.at[row], sems.at[row])
        for row, ref in enumerate((old_ref, new_ref))
    ]
    for copy in copies:
        copy.start()
    for copy in copies:
        copy.wait()
    pair = pair_index()
    block = 2 * pair + lax.axis_index("yl")
    facts = (
        offsets_ref[0, 2 * pair],
        offsets_ref[0, 2 * pair + 1],
        offsets_ref[0, 2 * pair + 2],
        offsets_ref[1, block],
        offsets_ref[1, block + 1],
    )
    for row, fact in enumerate(facts):
        facts_ref[row : row + 1, :] = jnp.full((1, HEAD), fact, jnp.int32)
    facts_ref[len(facts) :, :] = jnp.zeros((8 - len(facts), HEAD), jnp.int32)


def raw_rows(facts_ref, slots_ref):
    place = lax.broadcasted_iota(jnp.int32, (SPAN, 1), 0) + (pair_index() * PAIR - LEAD)
    first = facts_ref[0:1, 0:1]
    middle = facts_ref[1:2, 0:1]
    last = facts_ref[2:3, 0:1]
    source = jnp.where(place < middle, place - first, SLOTS + place - middle)
    source = jnp.where((place >= first) & (place < last), source, -1)
    return picked(SPAN, source, slots_ref[...])


def raw_keys_kernel(facts_ref, slots_ref, out_ref):
    out_ref[...] = raw_rows(facts_ref, slots_ref)


def raw_queries_kernel(facts_ref, slots_ref, edge_ref, rows_ref):
    rows = raw_rows(facts_ref, slots_ref)
    edge_ref[...] = rows[PAIR:]
    rows_ref[...] = rows[:PAIR]


def joined(rows, edge):
    return jnp.concatenate([rows[:EDGE] + edge, rows[EDGE:]], axis=0)


def relay_kernel(mine_ref, first_ref, second_ref, fourth_ref):
    whole = joined(mine_ref[:PAIR], first_ref[PAIR:SPAN])
    edge = mine_ref[PAIR:SPAN]
    second_ref[:PAIR] = whole
    second_ref[PAIR:SPAN] = edge
    second_ref[SPAN:] = first_ref[:PAIR]
    fourth_ref[:PAIR] = whole
    fourth_ref[PAIR:] = edge


def attend_kernel(
    rows_ref, edge_ref, extra_ref, mine_ref, first_ref, second_ref, fourth_ref,
    out_ref, edge_out_ref, extra_out_ref, kept_ref, near_ref, past_ref, give2_ref, give4_ref,
    score_ref,
):
    pair = pair_index()
    main = 2 * PAIR
    width = main + 2 * EXTRA
    own = mine_ref[:PAIR]
    past = mine_ref[PAIR : PAIR + EXTRA]
    far = fourth_ref[:PAIR]
    others = (
        joined(first_ref[:PAIR], second_ref[PAIR:SPAN]),
        second_ref[:PAIR],
        joined(second_ref[SPAN:], fourth_ref[PAIR:]),
    )
    used = jnp.where(pair == PAIRS - 1, 1.0, 0.0).astype(jnp.bfloat16)

    def stacked(column):
        parts, extras = [], []
        for head in range(2):
            columns = slice(column + head * HEAD, column + (head + 1) * HEAD)
            parts.append(joined(rows_ref[:, columns], edge_ref[:, columns]))
            extras.append(extra_ref[:EXTRA, columns] * used)
        return jnp.concatenate(parts + extras, axis=0)

    queries = stacked(0)
    grads = stacked(2 * HEAD)
    key_row = lax.broadcasted_iota(jnp.int32, (PAIR, width), 0)
    lane = lax.broadcasted_iota(jnp.int32, (PAIR, width), 1)
    near = key_row <= jnp.where(lane < main, lane & (PAIR - 1), PAIR)
    past_row = lax.broadcasted_iota(jnp.int32, (EXTRA, 2 * EXTRA), 0)
    past_lane = lax.broadcasted_iota(jnp.int32, (EXTRA, 2 * EXTRA), 1)
    beyond = past_row <= (past_lane & (EXTRA - 1))
    place = lax.broadcasted_iota(jnp.int32, (PAIR, 1), 0) + (pair * PAIR - LEAD)

    def scores(keys, distance):
        bias = jnp.where(place - distance * PAIR >= 0, 0.0, OUTSIDE)
        return dot(keys[:, :HEAD], queries, NT) * (SCALE * LOG2E) + bias

    corner = (slice(2 * PAIR, 2 * PAIR + EXTRA), slice(main, width))
    for step, keys in enumerate(others):
        score_ref[step * PAIR : (step + 1) * PAIR, :] = scores(keys, step + 1)
    past_score = dot(past[:, :HEAD], queries[main:], NT) * (SCALE * LOG2E)
    score_ref[corner] = jnp.where(beyond, past_score, score_ref[corner])
    score_ref[3 * PAIR :, :] = jnp.where(near, scores(own, 0), scores(far, UNITS))
    top = jnp.full((1, width), OUTSIDE, jnp.float32)
    for step in range(UNITS):
        score = score_ref[step * PAIR : (step + 1) * PAIR, :]
        top = jnp.maximum(top, jnp.max(score, axis=0, keepdims=True))
    total = jnp.zeros((1, width), jnp.float32)
    for step in range(UNITS):
        weight = jnp.exp2(score_ref[step * PAIR : (step + 1) * PAIR, :] - top)
        score_ref[step * PAIR : (step + 1) * PAIR, :] = weight
        total = total + jnp.sum(weight, axis=0, keepdims=True)
    share = 1.0 / total

    def keep(step, columns, value):
        rounded = value.astype(jnp.bfloat16)
        if step == 0:
            kept_ref[:, columns] = value
        elif step == 1:
            near_ref[:, columns] = value
            give2_ref[PAIR:SPAN, columns] = rounded[:EDGE]
        elif step == 2:
            give2_ref[:PAIR, columns] = rounded
        elif step == 3:
            give2_ref[SPAN:, columns] = rounded
            give4_ref[PAIR:, columns] = rounded[:EDGE]
        else:
            give4_ref[:PAIR, columns] = rounded

    def without_corner(value):
        left = value[:EXTRA, :main]
        right = jnp.where(beyond, 0.0, value[:EXTRA, main:])
        return jnp.concatenate(
            [jnp.concatenate([left, right], axis=1), value[EXTRA:]], axis=0
        )

    def widened(value):
        return jnp.concatenate([jnp.zeros((HEAD, main), jnp.float32), value], axis=1)

    key_columns = slice(0, HEAD)
    value_columns = slice(HEAD, 2 * HEAD)
    attn = jnp.zeros((HEAD, width), jnp.float32)
    for step, keys in enumerate(others):
        prob = score_ref[step * PAIR : (step + 1) * PAIR, :] * share
        if step == 2:
            prob = without_corner(prob)
        prob = prob.astype(jnp.bfloat16)
        attn = attn + dot(keys[:, HEAD:], prob, TN)
        keep(step + 1, value_columns, dot(prob, grads, NN))
    prob = score_ref[3 * PAIR :, :] * share
    prob_own = jnp.where(near, prob, 0.0).astype(jnp.bfloat16)
    prob_far = jnp.where(near, 0.0, prob).astype(jnp.bfloat16)
    prob_past = score_ref[corner] * share[:, main:]
    prob_past = jnp.where(beyond, prob_past, 0.0).astype(jnp.bfloat16)
    attn = attn + dot(own[:, HEAD:], prob_own, TN) + dot(far[:, HEAD:], prob_far, TN)
    attn = attn + widened(dot(past[:, HEAD:], prob_past, TN))
    keep(0, value_columns, dot(prob_own, grads, NN))
    keep(UNITS, value_columns, dot(prob_far, grads, NN))
    past_ref[:, value_columns] = dot(prob_past, grads[main:], NN)
    attn = attn.astype(jnp.bfloat16).astype(jnp.float32)
    delta = jnp.sum(attn * grads.astype(jnp.float32).T, axis=0, keepdims=True)

    def store(value, column):
        rows = value.T.astype(jnp.bfloat16)
        for head in range(2):
            columns = slice(column + head * HEAD, column + (head + 1) * HEAD)
            out_ref[:, columns] = rows[head * PAIR : (head + 1) * PAIR]
            edge_out_ref[:, columns] = rows[head * PAIR : head * PAIR + EDGE]
            start = main + head * EXTRA
            extra_out_ref[:, columns] = rows[start : start + EXTRA]

    store(attn, 0)
    scaled = share * SCALE
    query_grad = jnp.zeros((HEAD, width), jnp.float32)
    for step, keys in enumerate(others):
        prob = score_ref[step * PAIR : (step + 1) * PAIR, :] * scaled
        change = prob * (dot(keys[:, HEAD:], grads, NT) - delta)
        if step == 2:
            change = without_corner(change)
        change = change.astype(jnp.bfloat16)
        query_grad = query_grad + dot(keys[:, :HEAD], change, TN)
        keep(step + 1, key_columns, dot(change, queries, NN))
    prob = score_ref[3 * PAIR :, :] * scaled
    grad_prob = jnp.where(near, dot(own[:, HEAD:], grads, NT), dot(far[:, HEAD:], grads, NT))
    change = prob * (grad_prob - delta)
    change_own = jnp.where(near, change, 0.0).astype(jnp.bfloat16)
    change_far = jnp.where(near, 0.0, change).astype(jnp.bfloat16)
    change = dot(past[:, HEAD:], grads[main:], NT) - delta[:, main:]
    change = jnp.where(beyond, score_ref[corner] * scaled[:, main:] * change, 0.0)
    change_past = change.astype(jnp.bfloat16)
    query_grad = query_grad + dot(own[:, :HEAD], change_own, TN)
    query_grad = query_grad + dot(far[:, :HEAD], change_far, TN)
    query_grad = query_grad + widened(dot(past[:, :HEAD], change_past, TN))
    keep(0, key_columns, dot(change_own, queries, NN))
    keep(UNITS, key_columns, dot(change_far, queries, NN))
    past_ref[:, key_columns] = dot(change_past, queries[main:], NN)
    store(query_grad, 2 * HEAD)


def merge_kernel(kept_ref, near_ref, past_ref, back2_ref, back4_ref, sum_ref, give_ref):
    def read(ref, start, rows):
        return ref[start : start + rows].astype(jnp.float32)

    sum_ref[:PAIR] = kept_ref[...] + read(back2_ref, 0, PAIR) + read(back4_ref, 0, PAIR)
    sum_ref[PAIR:] = read(back2_ref, PAIR, EDGE) + read(back4_ref, PAIR, EDGE)
    sum_ref[PAIR : PAIR + EXTRA] = sum_ref[PAIR : PAIR + EXTRA] + past_ref[...]
    give_ref[:PAIR] = (near_ref[...] + read(back2_ref, SPAN, PAIR)).astype(jnp.bfloat16)
    edge = kept_ref[:EDGE] + read(back2_ref, 0, EDGE) + read(back4_ref, 0, EDGE)
    give_ref[PAIR:] = edge.astype(jnp.bfloat16)


def swap_rows(out_ref, swap_ref):
    start = pl.multiple_of(jnp.where(lax.axis_index("yl") == 0, SPAN - SLOTS, 0), 16)
    swap_ref[...] = out_ref[pl.ds(start, SLOTS), :]


def span_kernel(rows_ref, edge_ref, extra_ref, out_ref, swap_ref):
    last = pair_index() == PAIRS - 1
    out_ref[:PAIR] = rows_ref[...]
    out_ref[PAIR : PAIR + EXTRA] = jnp.where(last, extra_ref[...], edge_ref[:EXTRA])
    out_ref[PAIR + EXTRA :] = edge_ref[EXTRA:]
    swap_rows(out_ref, swap_ref)


def total_kernel(sum_ref, back_ref, out_ref, swap_ref):
    out_ref[...] = (sum_ref[...] + back_ref[...].astype(jnp.float32)).astype(jnp.bfloat16)
    swap_rows(out_ref, swap_ref)


def place_kernel(facts_ref, rows_ref, swap_ref, first_ref, second_ref):
    start = facts_ref[3:4, 0:1]
    end = facts_ref[4:5, 0:1]
    slot = lax.broadcasted_iota(jnp.int32, (SLOTS, 1), 0)
    place = slot + (start - (pair_index() * PAIR - LEAD))
    live = slot < end - start
    partner_start = jnp.where(lax.axis_index("yl") == 0, 0, SPAN - SLOTS)
    own = picked(SLOTS, jnp.where(live, place, -1), rows_ref[...])
    other = picked(SLOTS, jnp.where(live, place - partner_start, -1), swap_ref[...])
    width = first_ref.shape[1] // 2

    def store(low, high):
        first_ref[:, :width] = low[:, :width]
        first_ref[:, width:] = high[:, :width]
        second_ref[:, :width] = low[:, width:]
        second_ref[:, width:] = high[:, width:]

    @pl.when(compute_member() == 0)
    def _():
        store(own, other)

    @pl.when(compute_member() == 1)
    def _():
        store(other, own)


def placed(facts, rows, swapped):
    width = rows.shape[1]
    return call(place_kernel, [shape(SLOTS, width)] * 2, [vmem()] * 3)(facts, rows, swapped)


def swapped(value):
    return lax.ppermute(value, "yl", [(0, 1), (1, 0)])


def shifted(value, steps):
    route = [
        (2 * pair + member, 2 * (pair + steps) + (member ^ (steps & 1)))
        for pair in range(max(0, -steps), min(PAIRS, PAIRS - steps))
        for member in range(2)
    ]
    return lax.ppermute(value, SEQ_AXES, route)


def layer(q_old, k_old, value_old_layout, dout_old, old_offsets, new_offsets):
    wide, narrow = 4 * HEAD, 2 * HEAD
    hbm = pl.BlockSpec(memory_space=pltpu.HBM)
    copies = [pltpu.SemaphoreType.DMA((16,))]
    packed_keys = call(
        pack_kernel, shape(8, 56, narrow), [hbm] * 2, copies, limit=60
    )(k_old, value_old_layout)
    packed_queries = call(
        pack_kernel, shape(8, 56, wide), [hbm] * 2, copies, limit=60
    )(q_old, dout_old)
    facts = call(
        facts_kernel,
        shape(8, HEAD, dtype=jnp.int32),
        [hbm] * 2,
        [
            pltpu.SMEM((2, old_offsets.shape[0]), jnp.int32),
            pltpu.SemaphoreType.DMA((2,)),
        ],
    )(old_offsets, new_offsets)
    key_slots = lax.all_to_all(packed_keys, GROUP_AXES, 0, 0, tiled=True)
    query_slots = lax.all_to_all(packed_queries, GROUP_AXES, 0, 0, tiled=True)
    first = call(raw_keys_kernel, shape(SPAN, narrow), [vmem()] * 2)(
        facts, key_slots.reshape(2 * SLOTS, narrow)
    )
    edge, rows = call(
        raw_queries_kernel, [shape(EDGE, wide), shape(PAIR, wide)], [vmem()] * 2
    )(facts, query_slots.reshape(2 * SLOTS, wide))
    from_first = shifted(first, 1)
    from_edge = shifted(edge, 1)
    second, fourth = call(
        relay_kernel, [shape(SPAN + PAIR, narrow), shape(SPAN, narrow)], [vmem()] * 2
    )(first, from_first)
    from_second = shifted(second, 2)
    from_fourth = shifted(fourth, 4)
    results, result_edge, result_extra, kept, near, past, give2, give4 = call(
        attend_kernel,
        [
            shape(PAIR, wide),
            shape(EDGE, wide),
            shape(EXTRA, wide),
            shape(PAIR, narrow, dtype=jnp.float32),
            shape(PAIR, narrow, dtype=jnp.float32),
            shape(EXTRA, narrow, dtype=jnp.float32),
            shape(SPAN + PAIR, narrow),
            shape(SPAN, narrow),
        ],
        [vmem()] * 7,
        [pltpu.VMEM((UNITS * PAIR, 2 * (PAIR + EXTRA)), jnp.float32)],
        flops=10**9,
        limit=24,
    )(rows, from_edge, edge, second, from_first, from_second, from_fourth)
    back2 = shifted(give2, -2)
    back4 = shifted(give4, -4)
    back_edge = shifted(result_edge, -1)
    sums, give = call(
        merge_kernel, [shape(SPAN, narrow, dtype=jnp.float32), shape(SPAN, narrow)], [vmem()] * 5
    )(kept, near, past, back2, back4)
    back = shifted(give, -1)
    span_rows, row_swap = call(
        span_kernel, [shape(SPAN, wide), shape(SLOTS, wide)], [vmem()] * 3
    )(results, back_edge, result_extra)
    other_rows = swapped(row_swap)
    totals, total_swap = call(
        total_kernel, [shape(SPAN, narrow), shape(SLOTS, narrow)], [vmem()] * 2
    )(sums, back)
    other_totals = swapped(total_swap)
    attn_out, grad_query_out = placed(facts, span_rows, other_rows)
    grad_key_out, grad_value_out = placed(facts, totals, other_totals)
    return attn_out, grad_query_out, grad_key_out, grad_value_out


def solution(mesh):
    cut = Mesh(mesh.devices.reshape(16, 2, 2, 2, 2, 2), AXES)
    rows = P(AXES, None)
    return jax.shard_map(
        layer,
        mesh=cut,
        in_specs=(rows, rows, rows, rows, P(), P()),
        out_specs=(P(SEQ_AXES, ("xl", "c")),) * 4,
        check_vma=False,
    )
```

```python
import jax
import jax.numpy as jnp
from jax import lax
from jax.experimental import pallas as pl
from jax.experimental.pallas import tpu as pltpu
from jax.sharding import Mesh, PartitionSpec as P


PAIR = 256
SLOTS = 224
LEAD = 48
EXTRA = 64
HALF = PAIR // 2
EDGE = 96
SPAN = PAIR + EDGE
HEAD = 128
UNITS = 4
PAIRS = 64
SCALE = 168.0 ** (-0.5)
LOG2E = 1.4426950408889634
OUTSIDE = -1e30

AXES = ("z", "xh", "yh", "yl", "xl", "c")
SEQ_AXES = ("z", "xh", "yh", "yl")
GROUP_AXES = ("yl", "xl", "c")

NT = (((1,), (1,)), ((), ()))
NN = (((1,), (0,)), ((), ()))
TN = (((0,), (0,)), ((), ()))


def dot(a, b, dims):
    return lax.dot_general(a, b, dims, preferred_element_type=jnp.float32)


def pair_index():
    return (lax.axis_index("z") * 2 + lax.axis_index("xh")) * 2 + lax.axis_index("yh")


def vmem():
    return pl.BlockSpec(memory_space=pltpu.VMEM)


def call(kernel, outs, specs, scratch=(), flops=0, limit=4):
    many = isinstance(outs, (list, tuple))
    return pl.pallas_call(
        kernel,
        out_shape=outs,
        in_specs=specs,
        out_specs=[vmem() for _ in outs] if many else vmem(),
        scratch_shapes=list(scratch),
        compiler_params=pltpu.CompilerParams(vmem_limit_bytes=limit << 20),
        cost_estimate=pl.CostEstimate(flops=flops, bytes_accessed=1 << 20, transcendentals=0),
    )


def shape(*dims, dtype=jnp.bfloat16):
    return jax.ShapeDtypeStruct(dims, dtype)


def picked(rows, source, candidates):
    count = candidates.shape[0]
    columns = lax.broadcasted_iota(jnp.int32, (rows, count), 1)
    chosen = (columns == source).astype(jnp.float32).astype(jnp.bfloat16)
    return dot(chosen, candidates, NN).astype(jnp.bfloat16)


def compute_member():
    return lax.axis_index("yl") ^ lax.axis_index("yh")


def start_packing(refs, out_ref, sems):
    mirrored = lax.axis_index("yh")
    copies = []
    for target in range(8):
        head = (target % 4) * 2 + ((target // 4) ^ mirrored)
        begin = 0
        for ref in refs:
            width = ref.shape[1] // 8
            source = ref.at[:, pl.ds(pl.multiple_of(head * width, HEAD), width)]
            copy = pltpu.make_async_copy(
                source, out_ref.at[target, :, pl.ds(begin, width)], sems.at[len(copies)]
            )
            copy.start()
            copies.append(copy)
            begin += width
    return copies


def pack_kernel(first_ref, second_ref, out_ref, sems):
    for copy in start_packing((first_ref, second_ref), out_ref, sems):
        copy.wait()


def facts_kernel(old_ref, new_ref, facts_ref, offsets_ref, sems):
    copies = [
        pltpu.make_async_copy(ref, offsets_ref.at[row], sems.at[row])
        for row, ref in enumerate((old_ref, new_ref))
    ]
    for copy in copies:
        copy.start()
    for copy in copies:
        copy.wait()
    pair = pair_index()
    block = 2 * pair + lax.axis_index("yl")
    facts = (
        offsets_ref[0, 2 * pair],
        offsets_ref[0, 2 * pair + 1],
        offsets_ref[0, 2 * pair + 2],
        offsets_ref[1, block],
        offsets_ref[1, block + 1],
    )
    for row, fact in enumerate(facts):
        facts_ref[row : row + 1, :] = jnp.full((1, HEAD), fact, jnp.int32)
    facts_ref[len(facts) :, :] = jnp.zeros((8 - len(facts), HEAD), jnp.int32)


def raw_rows(facts_ref, slots_ref):
    place = lax.broadcasted_iota(jnp.int32, (SPAN, 1), 0) + (pair_index() * PAIR - LEAD)
    first = facts_ref[0:1, 0:1]
    middle = facts_ref[1:2, 0:1]
    last = facts_ref[2:3, 0:1]
    source = jnp.where(place < middle, place - first, SLOTS + place - middle)
    source = jnp.where((place >= first) & (place < last), source, -1)
    return picked(SPAN, source, slots_ref[...])


def raw_keys_kernel(facts_ref, slots_ref, out_ref):
    out_ref[...] = raw_rows(facts_ref, slots_ref)


def raw_queries_kernel(facts_ref, slots_ref, edge_ref, rows_ref):
    rows = raw_rows(facts_ref, slots_ref)
    edge_ref[...] = rows[PAIR:]
    rows_ref[...] = rows[:PAIR]


def joined(rows, edge):
    return jnp.concatenate([rows[:EDGE] + edge, rows[EDGE:]], axis=0)


def relay_kernel(mine_ref, first_ref, second_ref, fourth_ref):
    whole = joined(mine_ref[:PAIR], first_ref[PAIR:SPAN])
    edge = mine_ref[PAIR:SPAN]
    second_ref[:PAIR] = whole
    second_ref[PAIR:SPAN] = edge
    second_ref[SPAN:] = first_ref[:PAIR]
    fourth_ref[:PAIR] = whole
    fourth_ref[PAIR:] = edge


def attend(queries, grads, full, near_block, far_block, past, score_ref, give):
    width = queries.shape[0]
    near_keys, near_bias = near_block
    far_keys, far_bias = far_block
    starts = [0]
    for keys, _ in full:
        starts.append(starts[-1] + keys.shape[0])
    spans = [slice(low, high) for low, high in zip(starts, starts[1:])]
    mixed = slice(starts[-1], starts[-1] + HALF)
    lane = lax.broadcasted_iota(jnp.int32, (HALF, width), 1)
    row = lax.broadcasted_iota(jnp.int32, (HALF, width), 0)
    near = row <= jnp.where(lane < PAIR, lane & (HALF - 1), HALF)
    corner = (slice(starts[2], starts[2] + EXTRA), slice(PAIR, width))
    if past is not None:
        past_lane = lax.broadcasted_iota(jnp.int32, (EXTRA, width - PAIR), 1)
        past_row = lax.broadcasted_iota(jnp.int32, (EXTRA, width - PAIR), 0)
        beyond = past_row <= (past_lane & (EXTRA - 1))

    def scores(keys, bias):
        return dot(keys[:, :HEAD], queries, NT) * (SCALE * LOG2E) + bias

    def without_corner(value):
        left = value[:EXTRA, :PAIR]
        right = jnp.where(beyond, 0.0, value[:EXTRA, PAIR:])
        return jnp.concatenate([jnp.concatenate([left, right], axis=1), value[EXTRA:]], axis=0)

    def widened(value):
        return jnp.concatenate([jnp.zeros((HEAD, PAIR), jnp.float32), value], axis=1)

    for (keys, bias), span in zip(full, spans):
        score_ref[span, :] = scores(keys, bias)
    if past is not None:
        past_score = dot(past[:, :HEAD], queries[PAIR:], NT) * (SCALE * LOG2E)
        score_ref[corner] = jnp.where(beyond, past_score, score_ref[corner])
    score_ref[mixed, :] = jnp.where(near, scores(near_keys, near_bias), scores(far_keys, far_bias))
    top = jnp.full((1, width), OUTSIDE, jnp.float32)
    for span in spans + [mixed]:
        top = jnp.maximum(top, jnp.max(score_ref[span, :], axis=0, keepdims=True))
    total = jnp.zeros((1, width), jnp.float32)
    for span in spans + [mixed]:
        weight = jnp.exp2(score_ref[span, :] - top)
        score_ref[span, :] = weight
        total = total + jnp.sum(weight, axis=0, keepdims=True)
    share = 1.0 / total
    key_columns = slice(0, HEAD)
    value_columns = slice(HEAD, 2 * HEAD)
    attn = jnp.zeros((HEAD, width), jnp.float32)
    for index, ((keys, _), span) in enumerate(zip(full, spans)):
        prob = score_ref[span, :] * share
        if index == 2 and past is not None:
            prob = without_corner(prob)
        prob = prob.astype(jnp.bfloat16)
        attn = attn + dot(keys[:, HEAD:], prob, TN)
        give(index, value_columns, dot(prob, grads, NN))
    prob = score_ref[mixed, :] * share
    prob_near = jnp.where(near, prob, 0.0).astype(jnp.bfloat16)
    prob_far = jnp.where(near, 0.0, prob).astype(jnp.bfloat16)
    attn = attn + dot(near_keys[:, HEAD:], prob_near, TN) + dot(far_keys[:, HEAD:], prob_far, TN)
    give("near", value_columns, dot(prob_near, grads, NN))
    give("far", value_columns, dot(prob_far, grads, NN))
    if past is not None:
        prob_past = score_ref[corner] * share[:, PAIR:]
        prob_past = jnp.where(beyond, prob_past, 0.0).astype(jnp.bfloat16)
        attn = attn + widened(dot(past[:, HEAD:], prob_past, TN))
        give("past", value_columns, dot(prob_past, grads[PAIR:], NN))
    attn = attn.astype(jnp.bfloat16).astype(jnp.float32)
    delta = jnp.sum(attn * grads.astype(jnp.float32).T, axis=0, keepdims=True)
    scaled = share * SCALE
    query_grad = jnp.zeros((HEAD, width), jnp.float32)
    for index, ((keys, _), span) in enumerate(zip(full, spans)):
        change = score_ref[span, :] * scaled * (dot(keys[:, HEAD:], grads, NT) - delta)
        if index == 2 and past is not None:
            change = without_corner(change)
        change = change.astype(jnp.bfloat16)
        query_grad = query_grad + dot(keys[:, :HEAD], change, TN)
        give(index, key_columns, dot(change, queries, NN))
    grad_prob = jnp.where(
        near, dot(near_keys[:, HEAD:], grads, NT), dot(far_keys[:, HEAD:], grads, NT)
    )
    change = score_ref[mixed, :] * scaled * (grad_prob - delta)
    change_near = jnp.where(near, change, 0.0).astype(jnp.bfloat16)
    change_far = jnp.where(near, 0.0, change).astype(jnp.bfloat16)
    query_grad = query_grad + dot(near_keys[:, :HEAD], change_near, TN)
    query_grad = query_grad + dot(far_keys[:, :HEAD], change_far, TN)
    give("near", key_columns, dot(change_near, queries, NN))
    give("far", key_columns, dot(change_far, queries, NN))
    if past is not None:
        change = dot(past[:, HEAD:], grads[PAIR:], NT) - delta[:, PAIR:]
        change = jnp.where(beyond, score_ref[corner] * scaled[:, PAIR:] * change, 0.0)
        change = change.astype(jnp.bfloat16)
        query_grad = query_grad + widened(dot(past[:, :HEAD], change, TN))
        give("past", key_columns, dot(change, queries[PAIR:], NN))
    return attn.T.astype(jnp.bfloat16), query_grad.T.astype(jnp.bfloat16)


def key_units(mine_ref, first_ref, second_ref, fourth_ref):
    place = lax.broadcasted_iota(jnp.int32, (PAIR, 1), 0) + (pair_index() * PAIR - LEAD)
    units = (
        mine_ref[:PAIR],
        joined(first_ref[:PAIR], second_ref[PAIR:SPAN]),
        second_ref[:PAIR],
        joined(second_ref[SPAN:], fourth_ref[PAIR:]),
        fourth_ref[:PAIR],
    )
    return [
        (unit, jnp.where(place - distance * PAIR >= 0, 0.0, OUTSIDE))
        for distance, unit in enumerate(units)
    ]


def halves(unit):
    keys, bias = unit
    return (keys[:HALF], bias[:HALF]), (keys[HALF:], bias[HALF:])


def head_columns(base):
    return [slice(base + head * HEAD, base + (head + 1) * HEAD) for head in range(2)]


def late_kernel(
    rows_ref, extra_ref, mine_ref, first_ref, second_ref, fourth_ref,
    out_ref, extra_out_ref, sums_ref, past_ref, score_ref,
):
    units = key_units(mine_ref, first_ref, second_ref, fourth_ref)
    own_low, own_high = halves(units[0])
    _, far_high = halves(units[4])
    used = jnp.where(pair_index() == PAIRS - 1, 1.0, 0.0).astype(jnp.bfloat16)

    def stacked(base):
        parts = [rows_ref[HALF:, columns] for columns in head_columns(base)]
        parts += [extra_ref[:EXTRA, columns] * used for columns in head_columns(base)]
        return jnp.concatenate(parts, axis=0)

    def give(index, columns, value):
        if index == "past":
            past_ref[:, columns] = value
            return
        start = {0: 0, 1: PAIR, 2: 2 * PAIR, 3: 3 * PAIR, "near": 3 * PAIR + HALF, "far": 4 * PAIR}
        start = start[index]
        sums_ref[start : start + value.shape[0], columns] = value

    results = attend(
        stacked(0),
        stacked(2 * HEAD),
        [units[1], units[2], units[3], own_low],
        own_high,
        far_high,
        mine_ref[PAIR : PAIR + EXTRA],
        score_ref,
        give,
    )
    for base, value in zip((0, 2 * HEAD), results):
        for head, columns in enumerate(head_columns(base)):
            out_ref[:, columns] = value[head * HALF : (head + 1) * HALF]
            start = PAIR + head * EXTRA
            extra_out_ref[:, columns] = value[start : start + EXTRA]


def early_kernel(
    rows_ref, edge_ref, late_ref, sums_ref, mine_ref, first_ref, second_ref, fourth_ref,
    out_ref, edge_out_ref, kept_ref, near_ref, give2_ref, give4_ref, score_ref,
):
    units = key_units(mine_ref, first_ref, second_ref, fourth_ref)
    own_low, _ = halves(units[0])
    far_low, far_high = halves(units[4])

    def stacked(base):
        parts = [joined(rows_ref[:HALF, c], edge_ref[:, c]) for c in head_columns(base)]
        return jnp.concatenate(parts, axis=0)

    def give(index, columns, value):
        if index == "far":
            give4_ref[:HALF, columns] = value.astype(jnp.bfloat16)
            return
        start = {0: 0, 1: PAIR, 2: 2 * PAIR, 3: 4 * PAIR, "near": 3 * PAIR}[index]
        value = value + sums_ref[start : start + value.shape[0], columns]
        rounded = value.astype(jnp.bfloat16)
        if index == 0:
            near_ref[:, columns] = value
            give2_ref[PAIR:SPAN, columns] = rounded[:EDGE]
        elif index == 1:
            give2_ref[:PAIR, columns] = rounded
        elif index == 2:
            give2_ref[SPAN:, columns] = rounded
            give4_ref[PAIR:, columns] = rounded[:EDGE]
        elif index == 3:
            give4_ref[HALF:PAIR, columns] = rounded
        else:
            kept_ref[:HALF, columns] = value

    kept_ref[HALF:] = sums_ref[3 * PAIR + HALF : 4 * PAIR]
    results = attend(
        stacked(0),
        stacked(2 * HEAD),
        [units[1], units[2], units[3], far_high],
        own_low,
        far_low,
        None,
        score_ref,
        give,
    )
    for base, value in zip((0, 2 * HEAD), results):
        for head, columns in enumerate(head_columns(base)):
            part = value[head * HALF : (head + 1) * HALF]
            out_ref[:HALF, columns] = part
            edge_out_ref[:, columns] = part[:EDGE]
    out_ref[HALF:] = late_ref[...]


def merge_kernel(kept_ref, near_ref, past_ref, back2_ref, back4_ref, sum_ref, give_ref):
    def read(ref, start, rows):
        return ref[start : start + rows].astype(jnp.float32)

    sum_ref[:PAIR] = kept_ref[...] + read(back2_ref, 0, PAIR) + read(back4_ref, 0, PAIR)
    sum_ref[PAIR:] = read(back2_ref, PAIR, EDGE) + read(back4_ref, PAIR, EDGE)
    sum_ref[PAIR : PAIR + EXTRA] = sum_ref[PAIR : PAIR + EXTRA] + past_ref[...]
    give_ref[:PAIR] = (near_ref[...] + read(back2_ref, SPAN, PAIR)).astype(jnp.bfloat16)
    edge = kept_ref[:EDGE] + read(back2_ref, 0, EDGE) + read(back4_ref, 0, EDGE)
    give_ref[PAIR:] = edge.astype(jnp.bfloat16)


def swap_rows(out_ref, swap_ref):
    start = pl.multiple_of(jnp.where(lax.axis_index("yl") == 0, SPAN - SLOTS, 0), 16)
    swap_ref[...] = out_ref[pl.ds(start, SLOTS), :]


def span_kernel(rows_ref, edge_ref, extra_ref, out_ref, swap_ref):
    last = pair_index() == PAIRS - 1
    out_ref[:PAIR] = rows_ref[...]
    out_ref[PAIR : PAIR + EXTRA] = jnp.where(last, extra_ref[...], edge_ref[:EXTRA])
    out_ref[PAIR + EXTRA :] = edge_ref[EXTRA:]
    swap_rows(out_ref, swap_ref)


def total_kernel(sum_ref, back_ref, out_ref, swap_ref):
    out_ref[...] = (sum_ref[...] + back_ref[...].astype(jnp.float32)).astype(jnp.bfloat16)
    swap_rows(out_ref, swap_ref)


def place_kernel(facts_ref, rows_ref, swap_ref, first_ref, second_ref):
    start = facts_ref[3:4, 0:1]
    end = facts_ref[4:5, 0:1]
    slot = lax.broadcasted_iota(jnp.int32, (SLOTS, 1), 0)
    place = slot + (start - (pair_index() * PAIR - LEAD))
    live = slot < end - start
    partner_start = jnp.where(lax.axis_index("yl") == 0, 0, SPAN - SLOTS)
    own = picked(SLOTS, jnp.where(live, place, -1), rows_ref[...])
    other = picked(SLOTS, jnp.where(live, place - partner_start, -1), swap_ref[...])
    width = first_ref.shape[1] // 2

    def store(low, high):
        first_ref[:, :width] = low[:, :width]
        first_ref[:, width:] = high[:, :width]
        second_ref[:, :width] = low[:, width:]
        second_ref[:, width:] = high[:, width:]

    @pl.when(compute_member() == 0)
    def _():
        store(own, other)

    @pl.when(compute_member() == 1)
    def _():
        store(other, own)


def placed(facts, rows, swapped):
    width = rows.shape[1]
    return call(place_kernel, [shape(SLOTS, width)] * 2, [vmem()] * 3)(facts, rows, swapped)


def swapped(value):
    return lax.ppermute(value, "yl", [(0, 1), (1, 0)])


def shifted(value, steps):
    route = [
        (2 * pair + member, 2 * (pair + steps) + (member ^ (steps & 1)))
        for pair in range(max(0, -steps), min(PAIRS, PAIRS - steps))
        for member in range(2)
    ]
    return lax.ppermute(value, SEQ_AXES, route)


def layer(q_old, k_old, value_old_layout, dout_old, old_offsets, new_offsets):
    wide, narrow = 4 * HEAD, 2 * HEAD
    hbm = pl.BlockSpec(memory_space=pltpu.HBM)
    copies = [pltpu.SemaphoreType.DMA((16,))]
    packed_keys = call(
        pack_kernel, shape(8, 56, narrow), [hbm] * 2, copies, limit=60
    )(k_old, value_old_layout)
    packed_queries = call(
        pack_kernel, shape(8, 56, wide), [hbm] * 2, copies, limit=60
    )(q_old, dout_old)
    facts = call(
        facts_kernel,
        shape(8, HEAD, dtype=jnp.int32),
        [hbm] * 2,
        [
            pltpu.SMEM((2, old_offsets.shape[0]), jnp.int32),
            pltpu.SemaphoreType.DMA((2,)),
        ],
    )(old_offsets, new_offsets)
    key_slots = lax.all_to_all(packed_keys, GROUP_AXES, 0, 0, tiled=True)
    query_slots = lax.all_to_all(packed_queries, GROUP_AXES, 0, 0, tiled=True)
    first = call(raw_keys_kernel, shape(SPAN, narrow), [vmem()] * 2)(
        facts, key_slots.reshape(2 * SLOTS, narrow)
    )
    edge, rows = call(
        raw_queries_kernel, [shape(EDGE, wide), shape(PAIR, wide)], [vmem()] * 2
    )(facts, query_slots.reshape(2 * SLOTS, wide))
    from_first = shifted(first, 1)
    from_edge = shifted(edge, 1)
    second, fourth = call(
        relay_kernel, [shape(SPAN + PAIR, narrow), shape(SPAN, narrow)], [vmem()] * 2
    )(first, from_first)
    from_second = shifted(second, 2)
    from_fourth = shifted(fourth, 4)
    window = (second, from_first, from_second, from_fourth)
    late, result_extra, sums, past = call(
        late_kernel,
        [
            shape(HALF, wide),
            shape(EXTRA, wide),
            shape(4 * PAIR + HALF, narrow, dtype=jnp.float32),
            shape(EXTRA, narrow, dtype=jnp.float32),
        ],
        [vmem()] * 6,
        [pltpu.VMEM((UNITS * PAIR, PAIR + 2 * EXTRA), jnp.float32)],
        flops=10**9,
        limit=20,
    )(rows, edge, *window)
    results, result_edge, kept, near, give2, give4 = call(
        early_kernel,
        [
            shape(PAIR, wide),
            shape(EDGE, wide),
            shape(PAIR, narrow, dtype=jnp.float32),
            shape(PAIR, narrow, dtype=jnp.float32),
            shape(SPAN + PAIR, narrow),
            shape(SPAN, narrow),
        ],
        [vmem()] * 8,
        [pltpu.VMEM((UNITS * PAIR, PAIR), jnp.float32)],
        flops=10**9,
        limit=20,
    )(rows, from_edge, late, sums, *window)
    back2 = shifted(give2, -2)
    back4 = shifted(give4, -4)
    back_edge = shifted(result_edge, -1)
    totals_here, give = call(
        merge_kernel, [shape(SPAN, narrow, dtype=jnp.float32), shape(SPAN, narrow)], [vmem()] * 5
    )(kept, near, past, back2, back4)
    back = shifted(give, -1)
    span_rows, row_swap = call(
        span_kernel, [shape(SPAN, wide), shape(SLOTS, wide)], [vmem()] * 3
    )(results, back_edge, result_extra)
    other_rows = swapped(row_swap)
    totals, total_swap = call(
        total_kernel, [shape(SPAN, narrow), shape(SLOTS, narrow)], [vmem()] * 2
    )(totals_here, back)
    other_totals = swapped(total_swap)
    attn_out, grad_query_out = placed(facts, span_rows, other_rows)
    grad_key_out, grad_value_out = placed(facts, totals, other_totals)
    return attn_out, grad_query_out, grad_key_out, grad_value_out


def solution(mesh):
    cut = Mesh(mesh.devices.reshape(16, 2, 2, 2, 2, 2), AXES)
    rows = P(AXES, None)
    return jax.shard_map(
        layer,
        mesh=cut,
        in_specs=(rows, rows, rows, rows, P(), P()),
        out_specs=(P(SEQ_AXES, ("xl", "c")),) * 4,
        check_vma=False,
    )
```

```python
import jax
import jax.numpy as jnp
from jax import lax
from jax.experimental import pallas as pl
from jax.experimental.pallas import tpu as pltpu
from jax.sharding import Mesh, PartitionSpec as P


PAIR = 256
SLOTS = 224
LEAD = 48
EXTRA = 64
HALF = PAIR // 2
EDGE = 96
SPAN = PAIR + EDGE
HEAD = 128
UNITS = 4
PAIRS = 64
SCALE = 168.0 ** (-0.5)
LOG2E = 1.4426950408889634
OUTSIDE = -1e30

AXES = ("z", "xh", "yh", "yl", "xl", "c")
SEQ_AXES = ("z", "xh", "yh", "yl")
GROUP_AXES = ("yl", "xl", "c")

NT = (((1,), (1,)), ((), ()))
NN = (((1,), (0,)), ((), ()))
TN = (((0,), (0,)), ((), ()))


def dot(a, b, dims):
    return lax.dot_general(a, b, dims, preferred_element_type=jnp.float32)


def pair_index():
    return (lax.axis_index("z") * 2 + lax.axis_index("xh")) * 2 + lax.axis_index("yh")


def vmem():
    return pl.BlockSpec(memory_space=pltpu.VMEM)


def call(kernel, outs, specs, scratch=(), flops=0, limit=4):
    many = isinstance(outs, (list, tuple))
    return pl.pallas_call(
        kernel,
        out_shape=outs,
        in_specs=specs,
        out_specs=[vmem() for _ in outs] if many else vmem(),
        scratch_shapes=list(scratch),
        compiler_params=pltpu.CompilerParams(vmem_limit_bytes=limit << 20),
        cost_estimate=pl.CostEstimate(flops=flops, bytes_accessed=1 << 20, transcendentals=0),
    )


def shape(*dims, dtype=jnp.bfloat16):
    return jax.ShapeDtypeStruct(dims, dtype)


def picked(rows, source, candidates):
    count = candidates.shape[0]
    columns = lax.broadcasted_iota(jnp.int32, (rows, count), 1)
    chosen = (columns == source).astype(jnp.float32).astype(jnp.bfloat16)
    return dot(chosen, candidates, NN).astype(jnp.bfloat16)


def compute_member():
    return lax.axis_index("yl") ^ lax.axis_index("yh")


def start_packing(refs, out_ref, sems):
    mirrored = lax.axis_index("yh")
    copies = []
    for target in range(8):
        head = (target % 4) * 2 + ((target // 4) ^ mirrored)
        begin = 0
        for ref in refs:
            width = ref.shape[1] // 8
            source = ref.at[:, pl.ds(pl.multiple_of(head * width, HEAD), width)]
            copy = pltpu.make_async_copy(
                source, out_ref.at[target, :, pl.ds(begin, width)], sems.at[len(copies)]
            )
            copy.start()
            copies.append(copy)
            begin += width
    return copies


def pack_kernel(first_ref, second_ref, out_ref, sems):
    for copy in start_packing((first_ref, second_ref), out_ref, sems):
        copy.wait()


def facts_kernel(old_ref, new_ref, facts_ref, offsets_ref, sems):
    copies = [
        pltpu.make_async_copy(ref, offsets_ref.at[row], sems.at[row])
        for row, ref in enumerate((old_ref, new_ref))
    ]
    for copy in copies:
        copy.start()
    for copy in copies:
        copy.wait()
    pair = pair_index()
    block = 2 * pair + lax.axis_index("yl")
    facts = (
        offsets_ref[0, 2 * pair],
        offsets_ref[0, 2 * pair + 1],
        offsets_ref[0, 2 * pair + 2],
        offsets_ref[1, block],
        offsets_ref[1, block + 1],
    )
    for row, fact in enumerate(facts):
        facts_ref[row : row + 1, :] = jnp.full((1, HEAD), fact, jnp.int32)
    facts_ref[len(facts) :, :] = jnp.zeros((8 - len(facts), HEAD), jnp.int32)


def raw_rows(facts_ref, slots_ref, start, count):
    place = lax.broadcasted_iota(jnp.int32, (count, 1), 0) + (pair_index() * PAIR - LEAD + start)
    first = facts_ref[0:1, 0:1]
    middle = facts_ref[1:2, 0:1]
    last = facts_ref[2:3, 0:1]
    source = jnp.where(place < middle, place - first, SLOTS + place - middle)
    source = jnp.where((place >= first) & (place < last), source, -1)
    return picked(count, source, slots_ref[...])


def raw_keys_kernel(facts_ref, slots_ref, out_ref):
    out_ref[...] = raw_rows(facts_ref, slots_ref, 0, SPAN)


def raw_edge_kernel(facts_ref, slots_ref, edge_ref):
    edge_ref[...] = raw_rows(facts_ref, slots_ref, PAIR, EDGE)


def raw_queries_kernel(facts_ref, slots_ref, rows_ref):
    rows_ref[...] = raw_rows(facts_ref, slots_ref, 0, PAIR)


def joined(rows, edge):
    return jnp.concatenate([rows[:EDGE] + edge, rows[EDGE:]], axis=0)


def relay_kernel(mine_ref, first_ref, second_ref, fourth_ref):
    whole = joined(mine_ref[:PAIR], first_ref[PAIR:SPAN])
    edge = mine_ref[PAIR:SPAN]
    second_ref[:PAIR] = whole
    second_ref[PAIR:SPAN] = edge
    second_ref[SPAN:] = first_ref[:PAIR]
    fourth_ref[:PAIR] = whole
    fourth_ref[PAIR:] = edge


def attend(queries, grads, full, near_block, far_block, past, score_ref, give):
    width = queries.shape[0]
    near_keys, near_bias = near_block
    far_keys, far_bias = far_block
    starts = [0]
    for keys, _ in full:
        starts.append(starts[-1] + keys.shape[0])
    spans = [slice(low, high) for low, high in zip(starts, starts[1:])]
    mixed = slice(starts[-1], starts[-1] + HALF)
    lane = lax.broadcasted_iota(jnp.int32, (HALF, width), 1)
    row = lax.broadcasted_iota(jnp.int32, (HALF, width), 0)
    near = row <= jnp.where(lane < PAIR, lane & (HALF - 1), HALF)
    corner = (slice(starts[2], starts[2] + EXTRA), slice(PAIR, width))
    if past is not None:
        past_lane = lax.broadcasted_iota(jnp.int32, (EXTRA, width - PAIR), 1)
        past_row = lax.broadcasted_iota(jnp.int32, (EXTRA, width - PAIR), 0)
        beyond = past_row <= (past_lane & (EXTRA - 1))

    def scores(keys, bias):
        return dot(keys[:, :HEAD], queries, NT) * (SCALE * LOG2E) + bias

    def without_corner(value):
        left = value[:EXTRA, :PAIR]
        right = jnp.where(beyond, 0.0, value[:EXTRA, PAIR:])
        return jnp.concatenate([jnp.concatenate([left, right], axis=1), value[EXTRA:]], axis=0)

    def widened(value):
        return jnp.concatenate([jnp.zeros((HEAD, PAIR), jnp.float32), value], axis=1)

    for (keys, bias), span in zip(full, spans):
        score_ref[span, :] = scores(keys, bias)
    if past is not None:
        past_score = dot(past[:, :HEAD], queries[PAIR:], NT) * (SCALE * LOG2E)
        score_ref[corner] = jnp.where(beyond, past_score, score_ref[corner])
    score_ref[mixed, :] = jnp.where(near, scores(near_keys, near_bias), scores(far_keys, far_bias))
    top = jnp.full((1, width), OUTSIDE, jnp.float32)
    for span in spans + [mixed]:
        top = jnp.maximum(top, jnp.max(score_ref[span, :], axis=0, keepdims=True))
    total = jnp.zeros((1, width), jnp.float32)
    for span in spans + [mixed]:
        weight = jnp.exp2(score_ref[span, :] - top)
        score_ref[span, :] = weight
        total = total + jnp.sum(weight, axis=0, keepdims=True)
    share = 1.0 / total
    key_columns = slice(0, HEAD)
    value_columns = slice(HEAD, 2 * HEAD)
    attn = jnp.zeros((HEAD, width), jnp.float32)
    for index, ((keys, _), span) in enumerate(zip(full, spans)):
        prob = score_ref[span, :] * share
        if index == 2 and past is not None:
            prob = without_corner(prob)
        prob = prob.astype(jnp.bfloat16)
        attn = attn + dot(keys[:, HEAD:], prob, TN)
        give(index, value_columns, dot(prob, grads, NN))
    prob = score_ref[mixed, :] * share
    prob_near = jnp.where(near, prob, 0.0).astype(jnp.bfloat16)
    prob_far = jnp.where(near, 0.0, prob).astype(jnp.bfloat16)
    attn = attn + dot(near_keys[:, HEAD:], prob_near, TN) + dot(far_keys[:, HEAD:], prob_far, TN)
    give("near", value_columns, dot(prob_near, grads, NN))
    give("far", value_columns, dot(prob_far, grads, NN))
    if past is not None:
        prob_past = score_ref[corner] * share[:, PAIR:]
        prob_past = jnp.where(beyond, prob_past, 0.0).astype(jnp.bfloat16)
        attn = attn + widened(dot(past[:, HEAD:], prob_past, TN))
        give("past", value_columns, dot(prob_past, grads[PAIR:], NN))
    attn = attn.astype(jnp.bfloat16).astype(jnp.float32)
    delta = jnp.sum(attn * grads.astype(jnp.float32).T, axis=0, keepdims=True)
    scaled = share * SCALE
    query_grad = jnp.zeros((HEAD, width), jnp.float32)
    for index, ((keys, _), span) in enumerate(zip(full, spans)):
        change = score_ref[span, :] * scaled * (dot(keys[:, HEAD:], grads, NT) - delta)
        if index == 2 and past is not None:
            change = without_corner(change)
        change = change.astype(jnp.bfloat16)
        query_grad = query_grad + dot(keys[:, :HEAD], change, TN)
        give(index, key_columns, dot(change, queries, NN))
    grad_prob = jnp.where(
        near, dot(near_keys[:, HEAD:], grads, NT), dot(far_keys[:, HEAD:], grads, NT)
    )
    change = score_ref[mixed, :] * scaled * (grad_prob - delta)
    change_near = jnp.where(near, change, 0.0).astype(jnp.bfloat16)
    change_far = jnp.where(near, 0.0, change).astype(jnp.bfloat16)
    query_grad = query_grad + dot(near_keys[:, :HEAD], change_near, TN)
    query_grad = query_grad + dot(far_keys[:, :HEAD], change_far, TN)
    give("near", key_columns, dot(change_near, queries, NN))
    give("far", key_columns, dot(change_far, queries, NN))
    if past is not None:
        change = dot(past[:, HEAD:], grads[PAIR:], NT) - delta[:, PAIR:]
        change = jnp.where(beyond, score_ref[corner] * scaled[:, PAIR:] * change, 0.0)
        change = change.astype(jnp.bfloat16)
        query_grad = query_grad + widened(dot(past[:, :HEAD], change, TN))
        give("past", key_columns, dot(change, queries[PAIR:], NN))
    return attn.T.astype(jnp.bfloat16), query_grad.T.astype(jnp.bfloat16)


def key_units(mine_ref, first_ref, second_ref, fourth_ref):
    place = lax.broadcasted_iota(jnp.int32, (PAIR, 1), 0) + (pair_index() * PAIR - LEAD)
    units = (
        mine_ref[:PAIR],
        joined(first_ref[:PAIR], second_ref[PAIR:SPAN]),
        second_ref[:PAIR],
        joined(second_ref[SPAN:], fourth_ref[PAIR:]),
        fourth_ref[:PAIR],
    )
    return [
        (unit, jnp.where(place - distance * PAIR >= 0, 0.0, OUTSIDE))
        for distance, unit in enumerate(units)
    ]


def halves(unit):
    keys, bias = unit
    return (keys[:HALF], bias[:HALF]), (keys[HALF:], bias[HALF:])


def head_columns(base):
    return [slice(base + head * HEAD, base + (head + 1) * HEAD) for head in range(2)]


def late_kernel(
    rows_ref, extra_ref, mine_ref, first_ref, second_ref, fourth_ref,
    out_ref, extra_out_ref, sums_ref, past_ref, score_ref,
):
    units = key_units(mine_ref, first_ref, second_ref, fourth_ref)
    own_low, own_high = halves(units[0])
    _, far_high = halves(units[4])
    used = jnp.where(pair_index() == PAIRS - 1, 1.0, 0.0).astype(jnp.bfloat16)

    def stacked(base):
        parts = [rows_ref[HALF:, columns] for columns in head_columns(base)]
        parts += [extra_ref[:EXTRA, columns] * used for columns in head_columns(base)]
        return jnp.concatenate(parts, axis=0)

    def give(index, columns, value):
        if index == "past":
            past_ref[:, columns] = value
            return
        start = {0: 0, 1: PAIR, 2: 2 * PAIR, 3: 3 * PAIR, "near": 3 * PAIR + HALF, "far": 4 * PAIR}
        start = start[index]
        sums_ref[start : start + value.shape[0], columns] = value

    results = attend(
        stacked(0),
        stacked(2 * HEAD),
        [units[1], units[2], units[3], own_low],
        own_high,
        far_high,
        mine_ref[PAIR : PAIR + EXTRA],
        score_ref,
        give,
    )
    for base, value in zip((0, 2 * HEAD), results):
        for head, columns in enumerate(head_columns(base)):
            out_ref[:, columns] = value[head * HALF : (head + 1) * HALF]
            start = PAIR + head * EXTRA
            extra_out_ref[:, columns] = value[start : start + EXTRA]


def early_kernel(
    rows_ref, edge_ref, late_ref, sums_ref, mine_ref, first_ref, second_ref, fourth_ref,
    out_ref, edge_out_ref, kept_ref, near_ref, give2_ref, give4_ref, score_ref,
):
    units = key_units(mine_ref, first_ref, second_ref, fourth_ref)
    own_low, _ = halves(units[0])
    far_low, far_high = halves(units[4])

    def stacked(base):
        parts = [joined(rows_ref[:HALF, c], edge_ref[:, c]) for c in head_columns(base)]
        return jnp.concatenate(parts, axis=0)

    def give(index, columns, value):
        if index == "far":
            give4_ref[:HALF, columns] = value.astype(jnp.bfloat16)
            return
        start = {0: 0, 1: PAIR, 2: 2 * PAIR, 3: 4 * PAIR, "near": 3 * PAIR}[index]
        value = value + sums_ref[start : start + value.shape[0], columns]
        rounded = value.astype(jnp.bfloat16)
        if index == 0:
            near_ref[:, columns] = value
            give2_ref[PAIR:SPAN, columns] = rounded[:EDGE]
        elif index == 1:
            give2_ref[:PAIR, columns] = rounded
        elif index == 2:
            give2_ref[SPAN:, columns] = rounded
            give4_ref[PAIR:, columns] = rounded[:EDGE]
        elif index == 3:
            give4_ref[HALF:PAIR, columns] = rounded
        else:
            kept_ref[:HALF, columns] = value

    kept_ref[HALF:] = sums_ref[3 * PAIR + HALF : 4 * PAIR]
    results = attend(
        stacked(0),
        stacked(2 * HEAD),
        [units[1], units[2], units[3], far_high],
        own_low,
        far_low,
        None,
        score_ref,
        give,
    )
    for base, value in zip((0, 2 * HEAD), results):
        for head, columns in enumerate(head_columns(base)):
            part = value[head * HALF : (head + 1) * HALF]
            out_ref[:HALF, columns] = part
            edge_out_ref[:, columns] = part[:EDGE]
    out_ref[HALF:] = late_ref[...]


def merge_kernel(kept_ref, near_ref, past_ref, back2_ref, back4_ref, sum_ref, give_ref):
    def read(ref, start, rows):
        return ref[start : start + rows].astype(jnp.float32)

    sum_ref[:PAIR] = kept_ref[...] + read(back2_ref, 0, PAIR) + read(back4_ref, 0, PAIR)
    sum_ref[PAIR:] = read(back2_ref, PAIR, EDGE) + read(back4_ref, PAIR, EDGE)
    sum_ref[PAIR : PAIR + EXTRA] = sum_ref[PAIR : PAIR + EXTRA] + past_ref[...]
    give_ref[:PAIR] = (near_ref[...] + read(back2_ref, SPAN, PAIR)).astype(jnp.bfloat16)
    edge = kept_ref[:EDGE] + read(back2_ref, 0, EDGE) + read(back4_ref, 0, EDGE)
    give_ref[PAIR:] = edge.astype(jnp.bfloat16)


def swap_rows(out_ref, swap_ref):
    start = pl.multiple_of(jnp.where(lax.axis_index("yl") == 0, SPAN - SLOTS, 0), 16)
    swap_ref[...] = out_ref[pl.ds(start, SLOTS), :]


def span_kernel(rows_ref, edge_ref, extra_ref, out_ref, swap_ref):
    last = pair_index() == PAIRS - 1
    out_ref[:PAIR] = rows_ref[...]
    out_ref[PAIR : PAIR + EXTRA] = jnp.where(last, extra_ref[...], edge_ref[:EXTRA])
    out_ref[PAIR + EXTRA :] = edge_ref[EXTRA:]
    swap_rows(out_ref, swap_ref)


def total_kernel(sum_ref, back_ref, out_ref, swap_ref):
    out_ref[...] = (sum_ref[...] + back_ref[...].astype(jnp.float32)).astype(jnp.bfloat16)
    swap_rows(out_ref, swap_ref)


def place_kernel(facts_ref, rows_ref, swap_ref, first_ref, second_ref):
    start = facts_ref[3:4, 0:1]
    end = facts_ref[4:5, 0:1]
    slot = lax.broadcasted_iota(jnp.int32, (SLOTS, 1), 0)
    place = slot + (start - (pair_index() * PAIR - LEAD))
    live = slot < end - start
    partner_start = jnp.where(lax.axis_index("yl") == 0, 0, SPAN - SLOTS)
    own = picked(SLOTS, jnp.where(live, place, -1), rows_ref[...])
    other = picked(SLOTS, jnp.where(live, place - partner_start, -1), swap_ref[...])
    width = first_ref.shape[1] // 2

    def store(low, high):
        first_ref[:, :width] = low[:, :width]
        first_ref[:, width:] = high[:, :width]
        second_ref[:, :width] = low[:, width:]
        second_ref[:, width:] = high[:, width:]

    @pl.when(compute_member() == 0)
    def _():
        store(own, other)

    @pl.when(compute_member() == 1)
    def _():
        store(other, own)


def placed(facts, rows, swapped):
    width = rows.shape[1]
    return call(place_kernel, [shape(SLOTS, width)] * 2, [vmem()] * 3)(facts, rows, swapped)


def swapped(value):
    return lax.ppermute(value, "yl", [(0, 1), (1, 0)])


def shifted(value, steps):
    route = [
        (2 * pair + member, 2 * (pair + steps) + (member ^ (steps & 1)))
        for pair in range(max(0, -steps), min(PAIRS, PAIRS - steps))
        for member in range(2)
    ]
    return lax.ppermute(value, SEQ_AXES, route)


def layer(q_old, k_old, value_old_layout, dout_old, old_offsets, new_offsets):
    wide, narrow = 4 * HEAD, 2 * HEAD
    hbm = pl.BlockSpec(memory_space=pltpu.HBM)
    copies = [pltpu.SemaphoreType.DMA((16,))]
    packed_keys = call(
        pack_kernel, shape(8, 56, narrow), [hbm] * 2, copies, limit=60
    )(k_old, value_old_layout)
    packed_queries = call(
        pack_kernel, shape(8, 56, wide), [hbm] * 2, copies, limit=60
    )(q_old, dout_old)
    facts = call(
        facts_kernel,
        shape(8, HEAD, dtype=jnp.int32),
        [hbm] * 2,
        [
            pltpu.SMEM((2, old_offsets.shape[0]), jnp.int32),
            pltpu.SemaphoreType.DMA((2,)),
        ],
    )(old_offsets, new_offsets)
    key_slots = lax.all_to_all(packed_keys, GROUP_AXES, 0, 0, tiled=True)
    query_slots = lax.all_to_all(packed_queries, GROUP_AXES, 0, 0, tiled=True)
    first = call(raw_keys_kernel, shape(SPAN, narrow), [vmem()] * 2)(
        facts, key_slots.reshape(2 * SLOTS, narrow)
    )
    query_slots = query_slots.reshape(2 * SLOTS, wide)
    edge = call(raw_edge_kernel, shape(EDGE, wide), [vmem()] * 2)(facts, query_slots)
    rows = call(raw_queries_kernel, shape(PAIR, wide), [vmem()] * 2)(facts, query_slots)
    from_first = shifted(first, 1)
    from_edge = shifted(edge, 1)
    second, fourth = call(
        relay_kernel, [shape(SPAN + PAIR, narrow), shape(SPAN, narrow)], [vmem()] * 2
    )(first, from_first)
    from_second = shifted(second, 2)
    from_fourth = shifted(fourth, 4)
    window = (second, from_first, from_second, from_fourth)
    late, result_extra, sums, past = call(
        late_kernel,
        [
            shape(HALF, wide),
            shape(EXTRA, wide),
            shape(4 * PAIR + HALF, narrow, dtype=jnp.float32),
            shape(EXTRA, narrow, dtype=jnp.float32),
        ],
        [vmem()] * 6,
        [pltpu.VMEM((UNITS * PAIR, PAIR + 2 * EXTRA), jnp.float32)],
        flops=10**9,
        limit=20,
    )(rows, edge, *window)
    results, result_edge, kept, near, give2, give4 = call(
        early_kernel,
        [
            shape(PAIR, wide),
            shape(EDGE, wide),
            shape(PAIR, narrow, dtype=jnp.float32),
            shape(PAIR, narrow, dtype=jnp.float32),
            shape(SPAN + PAIR, narrow),
            shape(SPAN, narrow),
        ],
        [vmem()] * 8,
        [pltpu.VMEM((UNITS * PAIR, PAIR), jnp.float32)],
        flops=10**9,
        limit=20,
    )(rows, from_edge, late, sums, *window)
    back2 = shifted(give2, -2)
    back4 = shifted(give4, -4)
    back_edge = shifted(result_edge, -1)
    totals_here, give = call(
        merge_kernel, [shape(SPAN, narrow, dtype=jnp.float32), shape(SPAN, narrow)], [vmem()] * 5
    )(kept, near, past, back2, back4)
    back = shifted(give, -1)
    span_rows, row_swap = call(
        span_kernel, [shape(SPAN, wide), shape(SLOTS, wide)], [vmem()] * 3
    )(results, back_edge, result_extra)
    other_rows = swapped(row_swap)
    totals, total_swap = call(
        total_kernel, [shape(SPAN, narrow), shape(SLOTS, narrow)], [vmem()] * 2
    )(totals_here, back)
    other_totals = swapped(total_swap)
    attn_out, grad_query_out = placed(facts, span_rows, other_rows)
    grad_key_out, grad_value_out = placed(facts, totals, other_totals)
    return attn_out, grad_query_out, grad_key_out, grad_value_out


def solution(mesh):
    cut = Mesh(mesh.devices.reshape(16, 2, 2, 2, 2, 2), AXES)
    rows = P(AXES, None)
    return jax.shard_map(
        layer,
        mesh=cut,
        in_specs=(rows, rows, rows, rows, P(), P()),
        out_specs=(P(SEQ_AXES, ("xl", "c")),) * 4,
        check_vma=False,
    )
```
